32 devices in a mesh: gx: 8 (over y, x, core), gy: 4 (over z).
Axes of the slice: x: 2, y: 2, z: 4, core: 2. Of those that a mesh axis runs over, the one named last changes fastest.
Arguments:
- eastward: float32 [64, 512, 128], P('gx', 'gy'), may hold values from -6 to 6
- northward: float32 [64, 512, 128], P('gx', 'gy'), may hold values from -6 to 6
- vertical: float32 [64, 512, 128], P('gx', 'gy'), may hold values from -6 to 6
- pressure: float32 [64, 512, 128], P('gx', 'gy'), may hold values from -6 to 6
- theta: float32 [64, 512, 128], P('gx', 'gy'), may hold values from -6 to 6
- humidity: float32 [64, 512, 128], P('gx', 'gy'), may hold values from 0.95 to 1.07
- sound_speed: float32 [128], replicated, may hold values from 0.25 to 1
- radius_sq: float32 [64, 8, 64, 512], P(None, None, 'gx', 'gy'), may hold values from 0.25 to 4
- multiplicity: bfloat16 [64, 8, 64, 512], P(None, None, 'gx', 'gy'), may hold values from 0.5 to 2
- droplet_count: int32 [8, 64, 512], P(None, 'gx', 'gy'), may hold values from 0 to 64
Outputs:
- eastward_out: float32 [64, 512, 128], P('gx', 'gy')
- northward_out: float32 [64, 512, 128], P('gx', 'gy')
- vertical_out: float32 [64, 512, 128], P('gx', 'gy')
- pressure_out: float32 [64, 512, 128], P('gx', 'gy')
- theta_out: float32 [64, 512, 128], P('gx', 'gy')
- humidity_out: float32 [64, 512, 128], P('gx', 'gy')
- radius_out: float32 [64, 8, 64, 512], P(None, None, 'gx', 'gy')
- saturation_profile: float32 [128], replicated
The draws below stay inside these ranges and needn't reach their ends.
All inputs are finite; a program needn't handle non-finite values.
Results may differ from the reference program's by a relative error of at most 0.0003.
Values sent between devices are 32-bit elements; how exact they have to be, the bound alone decides.
No kernel may reach another device: no remote copies, remote signals or barrier semaphores. Data moves between devices by JAX's collectives and lax.ppermute only.
A program may use at most 64 MiB of HBM per device.

```python
import math
import jax
import jax.numpy as jnp
from jax import lax

NZ = 128
SLOTS = 64
CLOUD = 8
SUB = 3
CLOUD_BASE = 32
NX = 64
NY = 512


def draw_humidity(key, part):
    first, second = jax.random.split(jax.random.fold_in(key, 17))
    across = jnp.arange(NX, dtype=jnp.float32) / NX
    along = jnp.arange(NY, dtype=jnp.float32) / NY
    offsets = 0.3 * jnp.clip(jax.random.normal(second, (NZ,), jnp.float32), -1.0, 1.0)
    ramp = 0.5 + 0.5 * across[:, None, None] + 0.5 * along[None, :, None]
    noise = jnp.clip(jax.random.normal(first, (NX, NY, NZ), jnp.float32), -4.0, 4.0)
    return 1.0 + 0.01 * (ramp + offsets[None, None, :] + noise)


def set_ends(result, rng, smallest, largest):
    longest = result.shape.index(max(result.shape))
    spots = []
    for shift in (0, 1):
        where = [jax.random.randint(jax.random.fold_in(rng, axis), (), 0, length) for axis, length in enumerate(result.shape)]
        where[longest] = (where[longest] + shift) % result.shape[longest]
        spots.append(tuple(where))
    return result.at[spots[0]].set(smallest).at[spots[1]].set(largest)


def shard_levels(own_key, extent, shards, smallest, high):
    loudness = 1.0
    for axis_at, parts in shards:
        steps = jax.random.uniform(jax.random.fold_in(jax.random.fold_in(own_key, 6), axis_at), (parts,), jnp.float32, smallest / len(shards), high / len(shards))
        loudness = loudness * jnp.repeat(jnp.exp(steps), extent[axis_at] // parts).reshape((-1,) + (1,) * (len(extent) - 1 - axis_at))
    return loudness


def bell_draw(rng, dims, deviation, limit, shards=(), kind=jnp.bfloat16):
    entries = deviation * jax.random.normal(rng, dims, jnp.float32)
    if shards:
        entries = entries * shard_levels(rng, dims, shards, -0.22, 0.18)
    return jnp.clip(entries, -limit, limit).astype(kind)


def setup_inputs(seed: int = 0) -> dict:
    key_list = jax.random.split(jax.random.key(seed), 11)
    eastward = bell_draw(key_list[0], (NX, NY, NZ), 1.0, 6.0, ((0, 8), (1, 4)), jnp.float32)
    northward = bell_draw(key_list[1], (NX, NY, NZ), 1.0, 6.0, ((0, 8), (1, 4)), jnp.float32)
    vertical = bell_draw(key_list[2], (NX, NY, NZ), 1.0, 6.0, ((0, 8), (1, 4)), jnp.float32)
    pressure = bell_draw(key_list[3], (NX, NY, NZ), 1.0, 6.0, ((0, 8), (1, 4)), jnp.float32)
    theta = bell_draw(key_list[4], (NX, NY, NZ), 1.0, 6.0, ((0, 8), (1, 4)), jnp.float32)
    humidity = draw_humidity(jax.random.fold_in(key_list[10], 71), 0)
    sound_speed = jnp.clip(jnp.exp(jax.random.uniform(key_list[6], (NZ,), jnp.float32, math.log(0.25), math.log(1.0))), 0.25, 1.0)
    radius_sq = jnp.clip(0.25 + 3.75 * jax.random.uniform(key_list[7], (SLOTS, CLOUD, NX, NY), jnp.float32) ** shard_levels(key_list[7], (SLOTS, CLOUD, NX, NY), ((2, 8), (3, 4)), -0.2, 0.2), 0.25, 4.0)
    multiplicity = jnp.clip(jnp.exp(math.log(2.0) - 1.3862944 * jax.random.uniform(key_list[8], (SLOTS, CLOUD, NX, NY), jnp.float32) ** shard_levels(key_list[8], (SLOTS, CLOUD, NX, NY), ((2, 8), (3, 4)), -0.2, 0.2)), 0.5, 2.0).astype(jnp.bfloat16)
    droplet_count = set_ends(jax.random.randint(key_list[9], (CLOUD, NX, NY), 0, SLOTS + 1), jax.random.fold_in(key_list[9], 1), 0, SLOTS).astype(jnp.int32)
    return {"eastward": eastward, "northward": northward, "vertical": vertical, "pressure": pressure, "theta": theta, "humidity": humidity, "sound_speed": sound_speed, "radius_sq": radius_sq, "multiplicity": multiplicity, "droplet_count": droplet_count}


TIME_STEP = 1.0
BUOYANCY = 0.5
VAPOUR_SLOPE = 0.01
GROWTH_RATE = 25.0
RADIUS_FLOOR = 0.0625
MASS_FACTOR = 0.0004
LATENT_HEAT = 200.0

def column_matrix(sound_speed):
    levels = sound_speed.shape[0]
    rows = lax.broadcasted_iota(jnp.int32, (levels, levels), 0)
    cols = lax.broadcasted_iota(jnp.int32, (levels, levels), 1)
    inside = rows < levels - 1
    gradient = jnp.where(inside & (cols == rows + 1), 1.0, 0.0) - jnp.where(inside & (cols == rows), 1.0, 0.0)
    gradient = gradient.astype(jnp.float32)
    scaled = gradient * sound_speed[None, :]
    product = jnp.dot(scaled.astype(jnp.float32), gradient.T.astype(jnp.float32), precision=lax.Precision.HIGHEST, preferred_element_type=jnp.float32)
    return jnp.eye(levels, dtype=jnp.float32) + TIME_STEP * TIME_STEP * product

def column_update(pressure, vertical, heat, divergence, sound_speed, inverse):
    levels = pressure.shape[-1]
    interior = (lax.broadcasted_iota(jnp.int32, (levels,), 0) < levels - 1).astype(jnp.float32)
    explicit = pressure - TIME_STEP * sound_speed * divergence
    upward = jnp.concatenate([explicit[..., 1:] - explicit[..., :-1], jnp.zeros_like(explicit[..., :1])], axis=-1)
    source = interior * (vertical + TIME_STEP * BUOYANCY * heat) - TIME_STEP * upward
    flat = source.reshape(-1, levels)
    solved = jnp.dot(flat.astype(jnp.float32), inverse.astype(jnp.float32), precision=lax.Precision.HIGHEST, preferred_element_type=jnp.float32).reshape(source.shape)
    masked = solved * interior
    below = jnp.concatenate([jnp.zeros_like(masked[..., :1]), masked[..., :-1]], axis=-1)
    return (explicit - TIME_STEP * sound_speed * (masked - below), solved)

def reference(eastward, northward, vertical, pressure, theta, humidity, sound_speed, radius_sq, multiplicity, droplet_count):
    sat = humidity * jnp.exp(-VAPOUR_SLOPE * theta) - 1.0
    cloud = jnp.transpose(sat[:, :, CLOUD_BASE:CLOUD_BASE + CLOUD], (2, 0, 1))
    grown = jnp.maximum(radius_sq + GROWTH_RATE * cloud[None], RADIUS_FLOOR)
    live = lax.broadcasted_iota(jnp.int32, radius_sq.shape, 0) < droplet_count[None]
    mass = multiplicity.astype(jnp.float32) * (grown * jnp.sqrt(grown) - radius_sq * jnp.sqrt(radius_sq))
    change = MASS_FACTOR * lax.optimization_barrier(jnp.sum(jnp.where(live, mass, 0.0), axis=0))
    added = jnp.pad(jnp.transpose(change, (1, 2, 0)), ((0, 0), (0, 0), (CLOUD_BASE, NZ - CLOUD_BASE - CLOUD)))
    humidity_out = humidity - added
    theta_out = theta + LATENT_HEAT * added
    radius_out = jnp.where(live, grown, 0.0)
    percent = 100.0 * (humidity_out * jnp.exp(-VAPOUR_SLOPE * theta_out) - 1.0)
    saturation_profile = lax.optimization_barrier(jnp.mean(percent, axis=(0, 1)))
    theta_mean = lax.optimization_barrier(jnp.mean(theta_out, axis=(0, 1)))
    heat = theta_out - theta_mean
    inverse = jnp.linalg.inv(column_matrix(sound_speed))
    for substep in range(SUB):
        grad_east = (jnp.roll(pressure, -1, 0) - jnp.roll(pressure, 1, 0)) * 0.5
        grad_north = (jnp.roll(pressure, -1, 1) - jnp.roll(pressure, 1, 1)) * 0.5
        eastward = eastward - TIME_STEP * grad_east
        northward = northward - TIME_STEP * grad_north
        spread = (jnp.roll(eastward, -1, 0) - jnp.roll(eastward, 1, 0) + jnp.roll(northward, -1, 1) - jnp.roll(northward, 1, 1)) * 0.5
        pressure, vertical = column_update(pressure, vertical, heat, spread, sound_speed, inverse)
    return (eastward, northward, vertical, pressure, theta_out, humidity_out, radius_out, saturation_profile)
```

```python
import functools

import jax
import jax.numpy as jnp
from jax import lax
from jax.experimental import pallas as pl
from jax.experimental.pallas import tpu as pltpu
from jax.sharding import PartitionSpec as P

SUB = 3
BUOYANCY = 0.5
VAPOUR_SLOPE = 0.01
GROWTH_RATE = 25.0
RADIUS_FLOOR = 0.0625
MASS_FACTOR = 0.0004
LATENT_HEAT = 200.0
TERMS = 6
CHUNK = 8
GRANT = 24 * 1024 * 1024

VMEM = pl.BlockSpec(memory_space=pltpu.VMEM)


def exact_dot(a, b):
    return jnp.dot(a, b, precision=lax.Precision.HIGHEST, preferred_element_type=jnp.float32)


def power15(x):
    return x * x * lax.rsqrt(x)


def condense_kernel(
    sound_ref,
    theta_ref,
    humidity_ref,
    radius_ref,
    mult_ref,
    count_ref,
    theta_out,
    humidity_out,
    radius_out,
    sums_out,
    inverse_out,
    cloud,
    total,
    series,
    power,
):
    step, steps = (pl.program_id(0), pl.num_programs(0))
    rows, cols, levels = theta_ref.shape
    layers = count_ref.shape[0]
    lowest = levels // 4

    @pl.when(step == 0)
    def _():
        for i in range(rows):
            sat = humidity_ref[i] * jnp.exp(-VAPOUR_SLOPE * theta_ref[i]) - 1.0
            cloud[:, i, :] = GROWTH_RATE * sat.T[lowest : lowest + layers]
        total[...] = jnp.zeros_like(total)
        r = lax.broadcasted_iota(jnp.int32, (levels, levels), 0)
        k = lax.broadcasted_iota(jnp.int32, (levels, levels), 1)
        sound = jnp.broadcast_to(sound_ref[...], (levels, levels))
        upper = jnp.where((k == r + 1) & (k < levels - 1), -sound, 0.0)
        above = pltpu.roll(sound, levels - 1, 1)
        diagonal = jnp.where(k == r, jnp.where(k < levels - 1, 1.0 + sound + above, 1.0), 0.0)
        eye = jnp.where(k == r, 1.0, 0.0)
        residual = eye - (diagonal + upper + upper.T) * (1.0 / 3.0)
        series[...] = (eye + residual) * (1.0 / 3.0)
        power[...] = exact_dot(residual, residual)

    @pl.when((step > 0) & (step < TERMS))
    def _():
        old = series[...]
        series[...] = old + exact_dot(old, power[...])
        power[...] = exact_dot(power[...], power[...])

    for s in range(CHUNK):
        live = step * CHUNK + s < count_ref[...]
        radius = radius_ref[s]
        grown = jnp.maximum(radius + cloud[...], RADIUS_FLOOR)
        radius_out[s] = jnp.where(live, grown, 0.0)
        mass = mult_ref[s].astype(jnp.float32) * (power15(grown) - power15(radius))
        total[...] += jnp.where(live, mass, 0.0)

    @pl.when(step == steps - 1)
    def _():
        inverse_out[...] = series[...]
        percent_sum = jnp.zeros((cols, levels), jnp.float32)
        theta_sum = jnp.zeros((cols, levels), jnp.float32)
        for i in range(rows):
            change = MASS_FACTOR * total[:, i, :]
            added = jnp.concatenate(
                [
                    jnp.zeros((lowest, cols), jnp.float32),
                    change,
                    jnp.zeros((levels - lowest - layers, cols), jnp.float32),
                ],
                axis=0,
            ).T
            humid = humidity_ref[i] - added
            warm = theta_ref[i] + LATENT_HEAT * added
            humidity_out[i] = humid
            theta_out[i] = warm
            percent_sum += 100.0 * (humid * jnp.exp(-VAPOUR_SLOPE * warm) - 1.0)
            theta_sum += warm
        sums_out[0:1] = jnp.sum(percent_sum, axis=0, keepdims=True)
        sums_out[1:2] = jnp.sum(theta_sum, axis=0, keepdims=True)


def condense(sound, theta, humidity, radius_sq, multiplicity, count):
    slots = radius_sq.shape[0]
    levels = theta.shape[2]
    whole = lambda a: pl.BlockSpec(a.shape, lambda s: (0,) * a.ndim)
    part = pl.BlockSpec((CHUNK,) + radius_sq.shape[1:], lambda s: (s, 0, 0, 0))
    f32 = lambda *shape: jax.ShapeDtypeStruct(shape, jnp.float32)
    outs = (f32(*theta.shape), f32(*theta.shape), f32(*radius_sq.shape), f32(2, levels), f32(levels, levels))
    return pl.pallas_call(
        condense_kernel,
        grid=(slots // CHUNK,),
        in_specs=[whole(sound), whole(theta), whole(humidity), part, part, whole(count)],
        out_specs=[whole(outs[0]), whole(outs[1]), part, whole(outs[3]), whole(outs[4])],
        out_shape=outs,
        scratch_shapes=[
            pltpu.VMEM(radius_sq.shape[1:], jnp.float32),
            pltpu.VMEM(radius_sq.shape[1:], jnp.float32),
            pltpu.VMEM((levels, levels), jnp.float32),
            pltpu.VMEM((levels, levels), jnp.float32),
        ],
        compiler_params=pltpu.CompilerParams(
            dimension_semantics=("arbitrary",), vmem_limit_bytes=GRANT
        ),
        cost_estimate=pl.CostEstimate(
            flops=4_000_000_000, bytes_accessed=8_000_000, transcendentals=1_000_000
        ),
        name="condense",
    )(sound, theta, humidity, radius_sq, multiplicity, count)


def column_step(q, held, sound, inside, inverse):
    levels = q.shape[-1]
    source = inside * (held + q - pltpu.roll(q, levels - 1, 1))
    solved = exact_dot(source, inverse)
    masked = solved * inside
    return (q - sound * (masked - pltpu.roll(masked, 1, 1)), solved)


def substep_kernel(first, last, axes, columns, *refs):
    refs = list(refs)
    take = lambda n: [refs.pop(0) for _ in range(n)]
    sound_ref, inverse_ref, heat_ref, p_ref, u_ref, v_ref, w_ref = take(7)
    d_ref = None if first else refs.pop(0)
    xa, xb, ya, yb = take(4)
    sums_ref = refs.pop(0) if last else None
    u_out, v_out, w_out, p_out = take(4)
    if last:
        profile_out = refs.pop(0)
    else:
        d_out, sxa, sxb, sya, syb = take(5)
    wide, low, high = take(3)
    rows, cols, levels = p_ref.shape
    pad = 8
    even_x = lax.rem(lax.axis_index(axes[0]), 2) == 0
    even_y = lax.rem(lax.axis_index(axes[1]), 2) == 0
    low[...] = jnp.where(even_x, xb[...], xa[...])
    high[...] = jnp.where(even_x, xa[...], xb[...])
    wide[:, pad : pad + cols, :] = p_ref[...]
    for n in range(2):
        wide[:, pad - 2 + n, :] = jnp.where(even_y, yb[n], ya[n])
        wide[:, pad + cols + n, :] = jnp.where(even_y, ya[n], yb[n])
    sound = sound_ref[...]
    level = lax.broadcasted_iota(jnp.int32, (1, levels), 1)
    inside = (level < levels - 1).astype(jnp.float32)
    inverse = inverse_ref[...]
    if last:
        total = sums_ref[...] * (1.0 / columns)
        profile_out[...] = total[0:1]
        mean = jnp.broadcast_to(total[1:2], (8, levels))
        drift_p, drift_w = (jnp.zeros_like(mean), jnp.zeros_like(mean))
        for _ in range(SUB):
            drift_p, drift_w = column_step(
                drift_p, drift_w - BUOYANCY * mean, sound, inside, inverse
            )
        drift_p, drift_w = (drift_p[0:1], drift_w[0:1])

    def row(i):
        if i < 0:
            return low[i + 2]
        if i >= rows:
            return high[i - rows]
        return p_ref[i]

    for i in range(rows):
        p = p_ref[i]
        east = lambda n: wide[i, pad + n : pad + n + cols, :]
        u_out[i] = u_ref[i] - 0.5 * (row(i + 1) - row(i - 1))
        v_out[i] = v_ref[i] - 0.5 * (east(1) - east(-1))
        bend = 0.25 * ((row(i + 2) + row(i - 2)) + (east(2) + east(-2))) - p
        if first:
            spread = jnp.zeros_like(p)
            if i + 1 < rows:
                spread += u_ref[i + 1]
            if i > 0:
                spread -= u_ref[i - 1]
            j = lax.broadcasted_iota(jnp.int32, (cols, levels), 0)
            v = v_ref[i]
            spread += jnp.where(j < cols - 1, pltpu.roll(v, cols - 1, 0), 0.0)
            spread -= jnp.where(j > 0, pltpu.roll(v, 1, 0), 0.0)
            d = 0.5 * spread - bend
        else:
            d = d_ref[i] - bend
        new_p, new_w = column_step(
            p - sound * d, w_ref[i] + BUOYANCY * heat_ref[i], sound, inside, inverse
        )
        if last:
            new_p += drift_p
            new_w += drift_w
        else:
            d_out[i] = d
        p_out[i] = new_p
        w_out[i] = new_w
    if not last:
        up, down = (p_out[rows - 2 : rows], p_out[0:2])
        sxa[...] = jnp.where(even_x, up, down)
        sxb[...] = jnp.where(even_x, down, up)
        for n in range(2):
            up, down = (p_out[:, cols - 2 + n, :], p_out[:, n, :])
            sya[n] = jnp.where(even_y, up, down)
            syb[n] = jnp.where(even_y, down, up)


def substep(index, columns, sound, inverse, heat, state, halo, sums=None):
    first, last = (index == 0, index == SUB - 1)
    p = state[0]
    rows, cols, levels = p.shape
    f32 = lambda *shape: jax.ShapeDtypeStruct(shape, jnp.float32)
    outs = [f32(*p.shape)] * 4
    if last:
        outs += [f32(1, levels)]
    else:
        outs += [f32(*p.shape)] + [f32(2, cols, levels)] * 2 + [f32(2, rows, levels)] * 2
    args = [sound, inverse, heat, *state, *halo] + ([sums] if last else [])
    return pl.pallas_call(
        functools.partial(substep_kernel, first, last, ("gx", "gy"), columns),
        in_specs=[VMEM] * len(args),
        out_specs=[VMEM] * len(outs),
        out_shape=outs,
        scratch_shapes=[
            pltpu.VMEM((rows, cols + 16, levels), jnp.float32),
            pltpu.VMEM((2, cols, levels), jnp.float32),
            pltpu.VMEM((2, cols, levels), jnp.float32),
        ],
        compiler_params=pltpu.CompilerParams(vmem_limit_bytes=GRANT),
        cost_estimate=pl.CostEstimate(
            flops=1_000_000_000, bytes_accessed=6_000_000, transcendentals=0
        ),
        name=f"substep{index}",
    )(*args)


def swaps(count):
    near = [(i, i ^ 1) for i in range(count)]
    far = [(i, (i + 1) % count if i % 2 else (i - 1) % count) for i in range(count)]
    return near, far


def exchange(sends):
    xa, xb, ya, yb = sends
    near_x, far_x = swaps(lax.axis_size("gx"))
    near_y, far_y = swaps(lax.axis_size("gy"))
    return (
        lax.ppermute(xa, "gx", near_x),
        lax.ppermute(xb, "gx", far_x),
        lax.ppermute(ya, "gy", near_y),
        lax.ppermute(yb, "gy", far_y),
    )


def total_sum(value):
    for axis in ("gx", "gy"):
        count = lax.axis_size(axis)
        distance = 1
        while distance < count:
            value = value + lax.ppermute(value, axis, [(i, i ^ distance) for i in range(count)])
            distance *= 2
    return value


def local(
    eastward,
    northward,
    vertical,
    pressure,
    theta,
    humidity,
    sound_speed,
    radius_sq,
    multiplicity,
    droplet_count,
):
    columns = float(theta.shape[0] * theta.shape[1] * lax.axis_size("gx") * lax.axis_size("gy"))
    sound = sound_speed[None]
    p, u, v = (pressure, eastward, northward)
    even_x = lax.axis_index("gx") % 2 == 0
    even_y = lax.axis_index("gy") % 2 == 0
    up_x = jnp.stack([p[-2] + 2.0 * u[-1], p[-1]])
    down_x = jnp.stack([p[0], p[1] - 2.0 * u[0]])
    up_y = jnp.stack([p[:, -2] + 2.0 * v[:, -1], p[:, -1]])
    down_y = jnp.stack([p[:, 0], p[:, 1] - 2.0 * v[:, 0]])
    halo = exchange(
        (
            jnp.where(even_x, up_x, down_x),
            jnp.where(even_x, down_x, up_x),
            jnp.where(even_y, up_y, down_y),
            jnp.where(even_y, down_y, up_y),
        )
    )
    theta_out, humidity_out, radius_out, sums, inverse = condense(
        sound, theta, humidity, radius_sq, multiplicity, droplet_count
    )
    sums = total_sum(sums)
    state = (p, u, v, vertical)
    for index in range(SUB):
        done = index == SUB - 1
        results = substep(
            index, columns, sound, inverse, theta_out, state, halo, sums if done else None
        )
        u, v, w, p = results[:4]
        if not done:
            state = (p, u, v, w, results[4])
            halo = exchange(results[5:])
    profile = results[4][0]
    return (u, v, w, p, theta_out, humidity_out, radius_out, profile)


def solution(mesh):
    grid = P("gx", "gy", None)
    drops = P(None, None, "gx", "gy")
    return jax.shard_map(
        local,
        mesh=mesh,
        in_specs=(grid,) * 6 + (P(), drops, drops, P(None, "gx", "gy")),
        out_specs=(grid,) * 6 + (drops, P()),
        check_vma=False,
    )
```

```python
import functools

import jax
import jax.numpy as jnp
from jax import lax
from jax.experimental import pallas as pl
from jax.experimental.pallas import tpu as pltpu
from jax.sharding import PartitionSpec as P

SUB = 3
BUOYANCY = 0.5
VAPOUR_SLOPE = 0.01
GROWTH_RATE = 25.0
RADIUS_FLOOR = 0.0625
MASS_FACTOR = 0.0004
LATENT_HEAT = 200.0
TERMS = 6
CHUNK = 8
GRANT = 24 * 1024 * 1024
PAD = 8
SIDE = 20
EXTRA = 56

VMEM = pl.BlockSpec(memory_space=pltpu.VMEM)


def exact_dot(a, b):
    return jnp.dot(a, b, precision=lax.Precision.HIGHEST, preferred_element_type=jnp.float32)


def power15(x):
    return x * x * lax.rsqrt(x)


def column_step(q, held, sound, inside, inverse):
    levels = q.shape[-1]
    source = inside * (held + q - pltpu.roll(q, levels - 1, 1))
    solved = exact_dot(source, inverse)
    masked = solved * inside
    return (q - sound * (masked - pltpu.roll(masked, 1, 1)), solved)


def interior(levels):
    level = lax.broadcasted_iota(jnp.int32, (1, levels), 1)
    return (level < levels - 1).astype(jnp.float32)


def even(axis):
    return lax.rem(lax.axis_index(axis), 2) == 0


def clear_rim(wide, rows, cols):
    shape = wide.shape
    for r in (0, 1, rows + 2, rows + 3):
        wide[r] = jnp.zeros(shape[1:], jnp.float32)
    for r in range(2, rows + 2):
        wide[r, 0:PAD, :] = jnp.zeros((PAD, shape[2]), jnp.float32)
        wide[r, PAD + cols :, :] = jnp.zeros((PAD, shape[2]), jnp.float32)


def bend(wide, r, cols):
    east = lambda n: wide[r, PAD + n : PAD + n + cols, :]
    up = wide[r + 2, PAD : PAD + cols, :]
    down = wide[r - 2, PAD : PAD + cols, :]
    return 0.25 * ((up + down) + (east(2) + east(-2))) - east(0)


def inverse_series(step, sound_ref, series, power):
    levels = series.shape[0]

    @pl.when(step == 0)
    def _():
        r = lax.broadcasted_iota(jnp.int32, (levels, levels), 0)
        k = lax.broadcasted_iota(jnp.int32, (levels, levels), 1)
        sound = jnp.broadcast_to(sound_ref[...], (levels, levels))
        upper = jnp.where((k == r + 1) & (k < levels - 1), -sound, 0.0)
        above = pltpu.roll(sound, levels - 1, 1)
        diagonal = jnp.where(k == r, jnp.where(k < levels - 1, 1.0 + sound + above, 1.0), 0.0)
        eye = jnp.where(k == r, 1.0, 0.0)
        residual = eye - (diagonal + upper + upper.T) * (1.0 / 3.0)
        series[...] = (eye + residual) * (1.0 / 3.0)
        power[...] = exact_dot(residual, residual)

    @pl.when((step > 0) & (step < TERMS))
    def _():
        old = series[...]
        series[...] = old + exact_dot(old, power[...])
        power[...] = exact_dot(power[...], power[...])


def first_kernel(
    axes,
    sound_hbm,
    theta_hbm,
    humidity_hbm,
    radius_hbm,
    mult_hbm,
    count_hbm,
    p_hbm,
    u_hbm,
    v_hbm,
    w_hbm,
    theta_final,
    humidity_final,
    radius_final,
    sums_out,
    series,
    p1_out,
    p2_out,
    p3_out,
    w3_out,
    drift_out,
    xa_out,
    xb_out,
    ya_out,
    yb_out,
    edge_out,
    cloud,
    total,
    power,
    wide,
    w2_out,
    d2_out,
    sound_ref,
    theta_ref,
    humidity_ref,
    radius_all,
    mult_all,
    count_ref,
    p_ref,
    u_ref,
    v_ref,
    w_ref,
    theta_out,
    humidity_out,
    radius_out,
    sems,
    chunk_sems,
):
    steps = radius_all.shape[0] // CHUNK
    rows, cols, levels = theta_ref.shape
    layers = count_ref.shape[0]
    lowest = levels // 4
    pairs = (
        (theta_hbm, theta_ref),
        (humidity_hbm, humidity_ref),
        (sound_hbm, sound_ref),
        (count_hbm, count_ref),
        (p_hbm, p_ref),
        (u_hbm, u_ref),
        (v_hbm, v_ref),
        (w_hbm, w_ref),
        (theta_out, theta_final),
        (humidity_out, humidity_final),
    )
    moves = [pltpu.make_async_copy(x, y, sems.at[n]) for n, (x, y) in enumerate(pairs)]

    def chunk_move(x, y, kind, step):
        span = pl.ds(step * CHUNK, CHUNK)
        return pltpu.make_async_copy(x.at[span], y.at[span], chunk_sems.at[kind, step])

    for move in moves[:4]:
        move.start()
    for step in range(steps):
        chunk_move(radius_hbm, radius_all, 0, step).start()
        chunk_move(mult_hbm, mult_all, 1, step).start()
    for move in moves[4:8]:
        move.start()
    for move in moves[:4]:
        move.wait()
    for i in range(rows):
        sat = humidity_ref[i] * jnp.exp(-VAPOUR_SLOPE * theta_ref[i]) - 1.0
        cloud[:, i, :] = GROWTH_RATE * sat.T[lowest : lowest + layers]
    total[...] = jnp.zeros_like(total)

    @pl.loop(0, steps)
    def _(step):
        chunk_move(radius_hbm, radius_all, 0, step).wait()
        chunk_move(mult_hbm, mult_all, 1, step).wait()
        inverse_series(step, sound_ref, series, power)
        for n in range(CHUNK):
            s = step * CHUNK + n
            live = s < count_ref[...]
            radius = radius_all[s]
            grown = jnp.maximum(radius + cloud[...], RADIUS_FLOOR)
            radius_out[s] = jnp.where(live, grown, 0.0)
            mass = mult_all[s].astype(jnp.float32) * (power15(grown) - power15(radius))
            total[...] += jnp.where(live, mass, 0.0)
        chunk_move(radius_out, radius_final, 2, step).start()

    if True:
        percent_sum = jnp.zeros((cols, levels), jnp.float32)
        theta_sum = jnp.zeros((cols, levels), jnp.float32)
        for i in range(rows):
            change = MASS_FACTOR * total[:, i, :]
            added = jnp.concatenate(
                [
                    jnp.zeros((lowest, cols), jnp.float32),
                    change,
                    jnp.zeros((levels - lowest - layers, cols), jnp.float32),
                ],
                axis=0,
            ).T
            humid = humidity_ref[i] - added
            warm = theta_ref[i] + LATENT_HEAT * added
            humidity_out[i] = humid
            theta_out[i] = warm
            percent_sum += 100.0 * (humid * jnp.exp(-VAPOUR_SLOPE * warm) - 1.0)
            theta_sum += warm
        sums_out[0:1] = jnp.sum(percent_sum, axis=0, keepdims=True)
        sums_out[1:2] = jnp.sum(theta_sum, axis=0, keepdims=True)

        for move in moves[8:]:
            move.start()
        for move in moves[4:8]:
            move.wait()
        sound = sound_ref[...]
        inside = interior(levels)
        inverse = series[...]
        clear_rim(wide, rows, cols)
        for i in range(rows):
            wide[i + 2, PAD : PAD + cols, :] = p_ref[i]
        j = lax.broadcasted_iota(jnp.int32, (cols, levels), 0)
        for i in range(rows):
            spread = jnp.zeros((cols, levels), jnp.float32)
            if i + 1 < rows:
                spread += u_ref[i + 1]
            if i > 0:
                spread -= u_ref[i - 1]
            v = v_ref[i]
            spread += jnp.where(j < cols - 1, pltpu.roll(v, cols - 1, 0), 0.0)
            spread -= jnp.where(j > 0, pltpu.roll(v, 1, 0), 0.0)
            d = 0.5 * spread - bend(wide, i + 2, cols)
            p1, w1 = column_step(
                p_ref[i] - sound * d,
                w_ref[i] + BUOYANCY * theta_out[i],
                sound,
                inside,
                inverse,
            )
            d2_out[i] = d
            p1_out[i] = p1
            w2_out[i] = w1
        for i in range(rows):
            wide[i + 2, PAD : PAD + cols, :] = p1_out[i]
        for i in range(rows):
            d = d2_out[i] - bend(wide, i + 2, cols)
            p2, w2 = column_step(
                p1_out[i] - sound * d,
                w2_out[i] + BUOYANCY * theta_out[i],
                sound,
                inside,
                inverse,
            )
            d2_out[i] = d
            p2_out[i] = p2
            w2_out[i] = w2

        for i in range(rows):
            wide[i + 2, PAD : PAD + cols, :] = p2_out[i]
        for i in range(rows):
            d = d2_out[i] - bend(wide, i + 2, cols)
            p3_out[i], w3_out[i] = column_step(
                p2_out[i] - sound * d,
                w2_out[i] + BUOYANCY * theta_out[i],
                sound,
                inside,
                inverse,
            )
        r = lax.broadcasted_iota(jnp.int32, (levels, levels), 0)
        k = lax.broadcasted_iota(jnp.int32, (levels, levels), 1)
        push = jnp.where(k == r, -BUOYANCY, 0.0)
        drift_p, drift_w = (jnp.zeros_like(push), jnp.zeros_like(push))
        for _ in range(SUB):
            drift_p, drift_w = column_step(drift_p, drift_w + push, sound, inside, inverse)
        drift_out[:, 0:levels] = drift_p
        drift_out[:, levels:] = drift_w

        even_x, even_y = (even(axes[0]), even(axes[1]))
        for k, field in enumerate((p_ref, p1_out, p2_out)):
            for n in range(2):
                if k > 0:
                    up, down = (field[rows - 2 + n], field[n])
                    xa_out[2 * k + n] = jnp.where(even_x, up, down)
                    xb_out[2 * k + n] = jnp.where(even_x, down, up)
                up, down = (field[:, cols - 2 + n, :], field[:, n, :])
                ya_out[2 * k + n] = jnp.where(even_y, up, down)
                yb_out[2 * k + n] = jnp.where(even_y, down, up)
        up, down = (p_ref[rows - 2] + 2.0 * u_ref[rows - 1], p_ref[1] - 2.0 * u_ref[0])
        xa_out[0] = jnp.where(even_x, up, p_ref[0])
        xa_out[1] = jnp.where(even_x, p_ref[rows - 1], down)
        xb_out[0] = jnp.where(even_x, p_ref[0], up)
        xb_out[1] = jnp.where(even_x, down, p_ref[rows - 1])
        up, down = (v_ref[:, cols - 1, :], v_ref[:, 0, :])
        ya_out[6] = jnp.where(even_y, up, down)
        yb_out[6] = jnp.where(even_y, down, up)
        for m, i in enumerate((0, rows - 1)):
            up, down = (u_ref[i, cols - 2 : cols, :], u_ref[i, 0:2, :])
            ya_out[7, 2 * m : 2 * m + 2, :] = jnp.where(even_y, up, down)
            yb_out[7, 2 * m : 2 * m + 2, :] = jnp.where(even_y, down, up)
        far_up, far_down = ([], [])
        for side, c in ((far_up, cols - 4), (far_down, 2)):
            for n in range(2):
                line = lambda ref, i: ref[i, c + n : c + n + 1, :]
                side += [line(p_ref, 0), line(p_ref, 1) - 2.0 * line(u_ref, 0)]
            for n in range(2):
                line = lambda ref, i: ref[i, c + n : c + n + 1, :]
                side += [
                    line(p_ref, rows - 2) + 2.0 * line(u_ref, rows - 1),
                    line(p_ref, rows - 1),
                ]
        up, down = (jnp.concatenate(far_up, axis=0), jnp.concatenate(far_down, axis=0))
        ya_out[8, 0:8, :] = jnp.where(even_y, up, down)
        yb_out[8, 0:8, :] = jnp.where(even_y, down, up)
        for out in (ya_out, yb_out):
            out[7, 4:, :] = jnp.zeros((rows - 4, levels), jnp.float32)
            out[9] = jnp.zeros((rows, levels), jnp.float32)
            out[9, 0:2, :] = sums_out[...]
        for m, i in enumerate((0, rows - 2)):
            for n in range(2):
                edge_out[4 * m + n : 4 * m + n + 1, :] = v_ref[i + n, 0:1, :]
                edge_out[4 * m + 2 + n : 4 * m + 3 + n, :] = v_ref[i + n, cols - 1 : cols, :]
        for m, i in enumerate((1, rows - 2)):
            edge_out[8 + 4 * m : 10 + 4 * m, :] = p_ref[i, 0:2, :]
            edge_out[10 + 4 * m : 12 + 4 * m, :] = p_ref[i, cols - 2 : cols, :]
        for step in range(steps):
            chunk_move(radius_out, radius_final, 2, step).wait()
        for move in moves[8:]:
            move.wait()


def first(sound, theta, humidity, radius_sq, multiplicity, count, p, u, v, w):
    slots = radius_sq.shape[0]
    rows, cols, levels = theta.shape
    hbm = pl.BlockSpec(memory_space=pltpu.HBM)
    f32 = lambda *shape: jax.ShapeDtypeStruct(shape, jnp.float32)
    block = f32(*theta.shape)
    outs = (
        [block, block, f32(*radius_sq.shape), f32(2, levels), f32(levels, levels)]
        + [block] * 4
        + [f32(levels, 2 * levels)]
        + [f32(6, cols, levels)] * 2
        + [f32(10, rows, levels)] * 2
        + [f32(16, levels)]
    )
    local_block = pltpu.VMEM(theta.shape, jnp.float32)
    layer_block = pltpu.VMEM(radius_sq.shape[1:], jnp.float32)
    return pl.pallas_call(
        functools.partial(first_kernel, ("gx", "gy")),
        in_specs=[hbm] * 10,
        out_specs=[hbm] * 3 + [VMEM] * 12,
        out_shape=outs,
        scratch_shapes=[
            layer_block,
            layer_block,
            pltpu.VMEM((levels, levels), jnp.float32),
            pltpu.VMEM((rows + 4, cols + 2 * PAD, levels), jnp.float32),
            local_block,
            local_block,
            pltpu.VMEM(sound.shape, jnp.float32),
            local_block,
            local_block,
            pltpu.VMEM(radius_sq.shape, jnp.float32),
            pltpu.VMEM(multiplicity.shape, multiplicity.dtype),
            pltpu.VMEM(count.shape, count.dtype),
        ]
        + [local_block] * 6
        + [
            pltpu.VMEM(radius_sq.shape, jnp.float32),
            pltpu.SemaphoreType.DMA((10,)),
            pltpu.SemaphoreType.DMA((3, slots // CHUNK)),
        ],
        compiler_params=pltpu.CompilerParams(vmem_limit_bytes=GRANT),
        cost_estimate=pl.CostEstimate(
            flops=8_000_000_000, bytes_accessed=12_000_000, transcendentals=1_000_000
        ),
        name="condense_and_evolve",
    )(sound, theta, humidity, radius_sq, multiplicity, count, p, u, v, w)


def corner_kernel(axes, ya_ref, yb_ref, edge_ref, sums_ref, a_out, b_out, sums_out):
    even_x, even_y = (even(axes[0]), even(axes[1]))
    rows = ya_ref.shape[1]
    levels = ya_ref.shape[2]
    low = jnp.where(even_y, yb_ref[...], ya_ref[...])
    high = jnp.where(even_y, ya_ref[...], yb_ref[...])

    def put(at, up, down):
        size = up.shape[0]
        a_out[at : at + size, :] = jnp.where(even_x, up, down)
        b_out[at : at + size, :] = jnp.where(even_x, down, up)

    for m, side in enumerate((low, high)):
        at = SIDE * m
        for n in range(4):
            put(at + 2 * n, side[n, rows - 2 : rows], side[n, 0:2])
        put(at + 8, side[7, 2:4], side[7, 0:2])
        put(at + 10, side[6, rows - 2 : rows], side[6, 0:2])
        inner = (side[0] + 2.0 * side[6], side[1]) if m == 0 else (side[0], side[1] - 2.0 * side[6])
        for n in range(2):
            put(at + 12 + 2 * n, inner[n][rows - 4 : rows - 2], inner[n][2:4])
        put(at + 16, side[8, 4:8], side[8, 0:4])
    put(2 * SIDE, edge_ref[4:8, :], edge_ref[0:4, :])
    put(2 * SIDE + 4, edge_ref[12:16, :], edge_ref[8:12, :])
    both = sums_ref[...] + ya_ref[9, 0:2, :]
    put(2 * SIDE + 8, both, both)
    sums_out[...] = both
    rest = jnp.zeros((EXTRA - 2 * SIDE - 10, levels), jnp.float32)
    put(2 * SIDE + 10, rest, rest)


def corner(ya, yb, edge, sums):
    levels = ya.shape[2]
    out = jax.ShapeDtypeStruct((EXTRA, levels), jnp.float32)
    return pl.pallas_call(
        functools.partial(corner_kernel, ("gx", "gy")),
        in_specs=[VMEM] * 4,
        out_specs=[VMEM] * 3,
        out_shape=[out, out, jax.ShapeDtypeStruct(sums.shape, jnp.float32)],
        compiler_params=pltpu.CompilerParams(vmem_limit_bytes=GRANT),
        cost_estimate=pl.CostEstimate(flops=10_000_000, bytes_accessed=100_000, transcendentals=0),
        name="corner",
    )(ya, yb, edge, sums)


def cross(mu, field, rows, cols):
    for r in range(rows + 4):
        if r < 2 or rows <= r < rows + 2:
            mu[r] = 0.25 * field[r + 2]
        elif r < 4 or r >= rows + 2:
            mu[r] = 0.25 * field[r - 2]
        else:
            mu[r] = jnp.zeros(mu.shape[1:], jnp.float32)
    for c in range(2):
        for base in (PAD, PAD + cols):
            mu[:, base - 2 + c, :] += 0.25 * field[:, base + c, :]
            mu[:, base + c, :] += 0.25 * field[:, base - 2 + c, :]


def last_kernel(
    axes,
    columns,
    sound_ref,
    inverse_ref,
    p0_ref,
    u_ref,
    v_ref,
    p1_ref,
    p2_ref,
    p3_ref,
    w3_ref,
    xa,
    xb,
    ya,
    yb,
    ca,
    cb,
    drift_ref,
    sums_ref,
    u_out,
    v_out,
    w_out,
    p_out,
    profile_out,
    f0,
    f1,
    f2,
    mu,
    yp,
    yw,
    yd,
    urows,
    vcols,
):
    rows, cols, levels = p0_ref.shape
    ext = cols + 2 * PAD
    even_x, even_y = (even(axes[0]), even(axes[1]))
    sound = sound_ref[...]
    inside = interior(levels)
    inverse = inverse_ref[...]
    body = slice(PAD, PAD + cols)
    low_y = jnp.where(even_y, yb[...], ya[...])
    high_y = jnp.where(even_y, ya[...], yb[...])
    low_c = jnp.where(even_x, cb[...], ca[...])
    high_c = jnp.where(even_x, ca[...], cb[...])
    pick = lambda one, two, n: jnp.where(even_x, one[n], two[n])
    sides = ((low_y, PAD - 2), (high_y, PAD + cols))
    ends = ((low_c, 0, xb, xa), (high_c, rows + 2, xa, xb))

    for r in range(rows + 4):
        for f in (f0, f1, f2):
            f[r, 0:PAD, :] = jnp.zeros((PAD, levels), jnp.float32)
            f[r, PAD + cols :, :] = jnp.zeros((PAD, levels), jnp.float32)
    for k, (f, ref) in enumerate(((f0, p0_ref), (f1, p1_ref), (f2, p2_ref))):
        for i in range(rows):
            f[i + 2, body, :] = ref[i]
        for _, at, one, two in ends:
            for n in range(2):
                f[at + n, body, :] = pick(one, two, 2 * k + n)
        for side, at in sides:
            for n in range(2):
                f[2 : rows + 2, at + n, :] = side[2 * k + n]
        if k < 2:
            for corner_rows, at, _, _ in ends:
                for m, (_, c) in enumerate(sides):
                    for n in range(2):
                        start = SIDE * m + 4 * k + 2 * n
                        for e in range(2):
                            f[at + e, c + n : c + n + 1, :] = corner_rows[start + e : start + e + 1]
    virtual = []
    for m, (c_rows, at, one, two) in enumerate(ends):
        outer = at + m
        virtual.append(f0[outer, body, :])
        for n, c in enumerate((PAD, PAD + cols - 2)):
            start = 2 * SIDE + 4 + 2 * n
            f0[outer, c : c + 2, :] = c_rows[start : start + 2]
    urows[...] = jnp.zeros_like(urows)
    for m, (c_rows, at, one, two) in enumerate(ends):
        outer, inner = ((0, 1), (3, 2))[m]
        urows[inner, body, :] = u_ref[0 if m == 0 else rows - 1]
        for s, (side, c) in enumerate(sides):
            urows[outer, c : c + 2, :] = c_rows[SIDE * s + 8 : SIDE * s + 10]
            urows[inner, c : c + 2, :] = side[7, 2 * m : 2 * m + 2]
    for s, (side, c) in enumerate(sides):
        outer, inner = ((0, 1), (3, 2))[s]
        vcols[outer, 2 : rows + 2, :] = side[6]
        vcols[inner, 2 : rows + 2, :] = v_ref[:, 0 if s == 0 else cols - 1, :]
        for c_rows, at, _, _ in ends:
            vcols[outer, at : at + 2, :] = c_rows[SIDE * s + 10 : SIDE * s + 12]
            vcols[inner, at : at + 2, :] = c_rows[2 * SIDE + 2 * s : 2 * SIDE + 2 * s + 2]

    cross(mu, f0, rows, cols)
    mu[2, body, :] += 0.25 * (virtual[0] - f0[0, body, :])
    mu[rows + 1, body, :] += 0.25 * (virtual[1] - f0[rows + 3, body, :])
    mu[1] -= 0.5 * urows[1]
    mu[2] += 0.5 * urows[0]
    mu[rows + 1] -= 0.5 * urows[3]
    mu[rows + 2] += 0.5 * urows[2]
    mu[:, PAD - 1, :] -= 0.5 * vcols[1]
    mu[:, PAD, :] += 0.5 * vcols[0]
    mu[:, PAD + cols - 1, :] -= 0.5 * vcols[3]
    mu[:, PAD + cols, :] += 0.5 * vcols[2]
    for c_rows, at, row in ((low_c, 0, 2), (high_c, rows + 2, rows)):
        for s, c in enumerate((PAD - 4, PAD + cols + 2)):
            for n in range(2):
                start = SIDE * s + 16 + 2 * n
                for e in range(2):
                    mu[row + e, c + n : c + n + 1, :] = 0.25 * c_rows[start + e : start + e + 1]
    far = 0.25 * jnp.concatenate(
        [c_rows[SIDE * s + 12 : SIDE * s + 16] for c_rows in (low_c, high_c) for s in range(2)],
        axis=0,
    )
    far, _ = column_step(sound * far, jnp.zeros_like(far), sound, inside, inverse)
    far = 0.25 * far

    for r in range(rows + 4):
        if 4 <= r < rows:
            spans = (slice(0, 2 * PAD), slice(cols, ext))
            clear = jnp.zeros((cols - 2 * PAD, levels), jnp.float32)
            for y in (yp, yw, yd):
                y[r, 2 * PAD : cols, :] = clear
        else:
            spans = (slice(0, ext),)
        for span in spans:
            d = -mu[r, span, :]
            q = -sound * d
            yp[r, span, :], yw[r, span, :] = column_step(
                q, jnp.zeros_like(q), sound, inside, inverse
            )
            yd[r, span, :] = d
    cross(mu, f1, rows, cols)
    for r in range(rows + 4):
        y = yp[r]
        near = pltpu.roll(y, 2, 0) + pltpu.roll(y, ext - 2, 0)
        if r >= 2:
            near += yp[r - 2]
        if r < rows + 2:
            near += yp[r + 2]
        mu[r] += 0.25 * near - y
        f0[r] += f1[r] + y
    for m, at in enumerate((0, rows + 2)):
        for s, c in enumerate((PAD, PAD + cols - 2)):
            for n in range(2):
                start = 8 * m + 4 * s + 2 * n
                for e in range(2):
                    mu[at + e, c + n : c + n + 1, :] += far[start + e : start + e + 1]
    for r in range(rows + 4):
        d = yd[r] - mu[r]
        p, w = column_step(yp[r] - sound * d, yw[r], sound, inside, inverse)
        yd[r] = d
        yp[r] = p
        yw[r] = w
        f0[r] += f2[r] + p
    cross(mu, f2, rows, cols)
    total = sums_ref[...] * (1.0 / columns)
    profile_out[...] = total[0:1]
    mean = jnp.broadcast_to(total[1:2], (8, levels))
    drift = exact_dot(mean, drift_ref[...])
    drift_p, drift_w = (drift[0:1, 0:levels], drift[0:1, levels:])
    for i in range(rows):
        r = i + 2
        d = yd[r, body, :] - mu[r, body, :] - bend(yp, r, cols)
        p, w = column_step(
            yp[r, body, :] - sound * d, yw[r, body, :], sound, inside, inverse
        )
        p_out[i] = p3_ref[i] + p + drift_p
        w_out[i] = w3_ref[i] + w + drift_w
        u_out[i] = u_ref[i] - 0.5 * (f0[r + 1, body, :] - f0[r - 1, body, :])
        east = lambda n: f0[r, PAD + n : PAD + n + cols, :]
        v_out[i] = v_ref[i] - 0.5 * (east(1) - east(-1))


def last(columns, *args):
    rows, cols, levels = args[2].shape
    f32 = lambda *shape: jax.ShapeDtypeStruct(shape, jnp.float32)
    block = f32(rows, cols, levels)
    wide = pltpu.VMEM((rows + 4, cols + 2 * PAD, levels), jnp.float32)
    return pl.pallas_call(
        functools.partial(last_kernel, ("gx", "gy"), columns),
        in_specs=[VMEM] * len(args),
        out_specs=[VMEM] * 5,
        out_shape=[block] * 4 + [f32(1, levels)],
        scratch_shapes=[wide] * 7
        + [
            pltpu.VMEM((4, cols + 2 * PAD, levels), jnp.float32),
            pltpu.VMEM((4, rows + 4, levels), jnp.float32),
        ],
        compiler_params=pltpu.CompilerParams(vmem_limit_bytes=GRANT),
        cost_estimate=pl.CostEstimate(
            flops=3_000_000_000, bytes_accessed=6_000_000, transcendentals=0
        ),
        name="response",
    )(*args)


def swaps(count):
    near = [(i, i ^ 1) for i in range(count)]
    far = [(i, (i + 1) % count if i % 2 else (i - 1) % count) for i in range(count)]
    return near, far


def exchange(a, b, axis):
    near, far = swaps(lax.axis_size(axis))
    return lax.ppermute(a, axis, near), lax.ppermute(b, axis, far)


def total_sum(value):
    for axis in ("gx", "gy"):
        count = lax.axis_size(axis)
        distance = 2
        while distance < count:
            value = value + lax.ppermute(value, axis, [(i, i ^ distance) for i in range(count)])
            distance *= 2
    return value


def local(
    eastward,
    northward,
    vertical,
    pressure,
    theta,
    humidity,
    sound_speed,
    radius_sq,
    multiplicity,
    droplet_count,
):
    columns = float(theta.shape[0] * theta.shape[1] * lax.axis_size("gx") * lax.axis_size("gy"))
    sound = sound_speed[None]
    (
        theta_out,
        humidity_out,
        radius_out,
        sums,
        inverse,
        p1,
        p2,
        p3,
        w3,
        drift,
        xa,
        xb,
        ya,
        yb,
        edge,
    ) = first(
        *(
            pltpu.with_memory_space_constraint(x, pltpu.HBM)
            for x in (
                sound,
                theta,
                humidity,
                radius_sq,
                multiplicity,
                droplet_count,
                pressure,
                eastward,
                northward,
                vertical,
            )
        )
    )
    xa, xb = exchange(xa, xb, "gx")
    ya, yb = exchange(ya, yb, "gy")
    ca, cb, sums = corner(ya, yb, edge, sums)
    ca, cb = exchange(ca, cb, "gx")
    at = 2 * SIDE + 8
    sums = total_sum(sums + ca[at : at + 2])
    u, v, w, p, profile = last(
        columns,
        sound,
        inverse,
        pressure,
        eastward,
        northward,
        p1,
        p2,
        p3,
        w3,
        xa,
        xb,
        ya,
        yb,
        ca,
        cb,
        drift,
        sums,
    )
    return (u, v, w, p, theta_out, humidity_out, radius_out, profile[0])


def solution(mesh):
    grid = P("gx", "gy", None)
    drops = P(None, None, "gx", "gy")
    return jax.shard_map(
        local,
        mesh=mesh,
        in_specs=(grid,) * 6 + (P(), drops, drops, P(None, "gx", "gy")),
        out_specs=(grid,) * 6 + (drops, P()),
        check_vma=False,
    )
```

```python
import functools

import jax
import jax.numpy as jnp
from jax import lax
from jax.experimental import pallas as pl
from jax.experimental.pallas import tpu as pltpu
from jax.sharding import PartitionSpec as P

SUB = 3
BUOYANCY = 0.5
VAPOUR_SLOPE = 0.01
GROWTH_RATE = 25.0
RADIUS_FLOOR = 0.0625
MASS_FACTOR = 0.0004
LATENT_HEAT = 200.0
TERMS = 6
CHUNK = 8
GRANT = 24 * 1024 * 1024
PAD = 8
SIDE = 20
EXTRA = 56

VMEM = pl.BlockSpec(memory_space=pltpu.VMEM)


def exact_dot(a, b):
    return jnp.dot(a, b, precision=lax.Precision.HIGHEST, preferred_element_type=jnp.float32)


def power15(x):
    return x * x * lax.rsqrt(x)


def split(x):
    high = x.astype(jnp.bfloat16)
    return high, (x - high.astype(jnp.float32)).astype(jnp.bfloat16)


def stack_weights(inverse, weights):
    levels = inverse.shape[0]
    high, low = split(inverse)
    weights[0:levels, 0:levels] = high
    weights[0:levels, levels:] = low
    weights[levels:, 0:levels] = high
    weights[levels:, levels:] = jnp.zeros_like(low)


def split_dot(x, weights):
    levels = x.shape[-1]
    both = jnp.concatenate(split(x), axis=1)
    out = jnp.dot(both, weights, preferred_element_type=jnp.float32)
    return out[:, :levels] + out[:, levels:]


def column_step(q, held, sound, inside, weights):
    levels = q.shape[-1]
    source = q - pltpu.roll(q, levels - 1, 1)
    if held is not None:
        source = source + held
    solved = split_dot(inside * source, weights)
    masked = solved * inside
    return (q - sound * (masked - pltpu.roll(masked, 1, 1)), solved)


def interior(levels):
    level = lax.broadcasted_iota(jnp.int32, (1, levels), 1)
    return (level < levels - 1).astype(jnp.float32)


def even(axis):
    return lax.rem(lax.axis_index(axis), 2) == 0


def clear_rim(wide, rows, cols):
    shape = wide.shape
    for r in (0, 1, rows + 2, rows + 3):
        wide[r] = jnp.zeros(shape[1:], jnp.float32)
    for r in range(2, rows + 2):
        wide[r, 0:PAD, :] = jnp.zeros((PAD, shape[2]), jnp.float32)
        wide[r, PAD + cols :, :] = jnp.zeros((PAD, shape[2]), jnp.float32)


def bend(wide, r, cols):
    east = lambda n: wide[r, PAD + n : PAD + n + cols, :]
    up = wide[r + 2, PAD : PAD + cols, :]
    down = wide[r - 2, PAD : PAD + cols, :]
    return 0.25 * ((up + down) + (east(2) + east(-2))) - east(0)


def inverse_series(step, sound_ref, series, power):
    levels = series.shape[0]

    @pl.when(step == 0)
    def _():
        r = lax.broadcasted_iota(jnp.int32, (levels, levels), 0)
        k = lax.broadcasted_iota(jnp.int32, (levels, levels), 1)
        sound = jnp.broadcast_to(sound_ref[...], (levels, levels))
        upper = jnp.where((k == r + 1) & (k < levels - 1), -sound, 0.0)
        above = pltpu.roll(sound, levels - 1, 1)
        diagonal = jnp.where(k == r, jnp.where(k < levels - 1, 1.0 + sound + above, 1.0), 0.0)
        eye = jnp.where(k == r, 1.0, 0.0)
        residual = eye - (diagonal + upper + upper.T) * (1.0 / 3.0)
        series[...] = (eye + residual) * (1.0 / 3.0)
        power[...] = exact_dot(residual, residual)

    @pl.when((step > 0) & (step < TERMS))
    def _():
        old = series[...]
        series[...] = old + exact_dot(old, power[...])
        power[...] = exact_dot(power[...], power[...])


def first_kernel(
    axes,
    sound_hbm,
    theta_hbm,
    humidity_hbm,
    radius_hbm,
    mult_hbm,
    count_hbm,
    p_hbm,
    u_hbm,
    v_hbm,
    w_hbm,
    theta_final,
    humidity_final,
    radius_final,
    sums_out,
    weights,
    p1_out,
    p2_out,
    w2_out,
    d2_out,
    heat_out,
    xa_out,
    xb_out,
    ya_out,
    yb_out,
    edge_out,
    cloud,
    total,
    power,
    series,
    wide,
    sound_ref,
    theta_ref,
    humidity_ref,
    radius_all,
    mult_all,
    count_ref,
    p_ref,
    u_ref,
    v_ref,
    w_ref,
    humidity_out,
    radius_out,
    sems,
    chunk_sems,
):
    steps = radius_all.shape[0] // CHUNK
    rows, cols, levels = theta_ref.shape
    layers = count_ref.shape[0]
    lowest = levels // 4
    pairs = (
        (theta_hbm, theta_ref),
        (humidity_hbm, humidity_ref),
        (sound_hbm, sound_ref),
        (count_hbm, count_ref),
        (p_hbm, p_ref),
        (u_hbm, u_ref),
        (v_hbm, v_ref),
        (w_hbm, w_ref),
        (heat_out, theta_final),
        (humidity_out, humidity_final),
    )
    moves = [pltpu.make_async_copy(x, y, sems.at[n]) for n, (x, y) in enumerate(pairs)]

    def chunk_move(x, y, kind, step):
        span = pl.ds(step * CHUNK, CHUNK)
        return pltpu.make_async_copy(x.at[span], y.at[span], chunk_sems.at[kind, step])

    for move in moves[:4]:
        move.start()
    for step in range(steps):
        chunk_move(radius_hbm, radius_all, 0, step).start()
        chunk_move(mult_hbm, mult_all, 1, step).start()
    for move in moves[4:8]:
        move.start()
    for move in moves[:4]:
        move.wait()
    for i in range(rows):
        sat = humidity_ref[i] * jnp.exp(-VAPOUR_SLOPE * theta_ref[i]) - 1.0
        cloud[:, i, :] = GROWTH_RATE * sat.T[lowest : lowest + layers]
    total[...] = jnp.zeros_like(total)

    @pl.loop(0, steps)
    def _(step):
        chunk_move(radius_hbm, radius_all, 0, step).wait()
        chunk_move(mult_hbm, mult_all, 1, step).wait()
        inverse_series(step, sound_ref, series, power)
        for n in range(CHUNK):
            s = step * CHUNK + n
            live = s < count_ref[...]
            radius = radius_all[s]
            grown = jnp.maximum(radius + cloud[...], RADIUS_FLOOR)
            radius_out[s] = jnp.where(live, grown, 0.0)
            mass = mult_all[s].astype(jnp.float32) * (power15(grown) - power15(radius))
            total[...] += jnp.where(live, mass, 0.0)
        chunk_move(radius_out, radius_final, 2, step).start()

    percent_sum = jnp.zeros((cols, levels), jnp.float32)
    theta_sum = jnp.zeros((cols, levels), jnp.float32)
    for i in range(rows):
        change = MASS_FACTOR * total[:, i, :]
        added = jnp.concatenate(
            [
                jnp.zeros((lowest, cols), jnp.float32),
                change,
                jnp.zeros((levels - lowest - layers, cols), jnp.float32),
            ],
            axis=0,
        ).T
        humid = humidity_ref[i] - added
        warm = theta_ref[i] + LATENT_HEAT * added
        humidity_out[i] = humid
        heat_out[i] = warm
        percent_sum += 100.0 * (humid * jnp.exp(-VAPOUR_SLOPE * warm) - 1.0)
        theta_sum += warm
    sums_out[0:1] = jnp.sum(percent_sum, axis=0, keepdims=True)
    sums_out[1:2] = jnp.sum(theta_sum, axis=0, keepdims=True)

    for move in moves[8:]:
        move.start()
    for move in moves[4:8]:
        move.wait()
    sound = sound_ref[...]
    inside = interior(levels)
    stack_weights(series[...], weights)
    inverse = weights[...]
    clear_rim(wide, rows, cols)
    for i in range(rows):
        wide[i + 2, PAD : PAD + cols, :] = p_ref[i]
    j = lax.broadcasted_iota(jnp.int32, (cols, levels), 0)
    for i in range(rows):
        spread = jnp.zeros((cols, levels), jnp.float32)
        if i + 1 < rows:
            spread += u_ref[i + 1]
        if i > 0:
            spread -= u_ref[i - 1]
        v = v_ref[i]
        spread += jnp.where(j < cols - 1, pltpu.roll(v, cols - 1, 0), 0.0)
        spread -= jnp.where(j > 0, pltpu.roll(v, 1, 0), 0.0)
        d = 0.5 * spread - bend(wide, i + 2, cols)
        p1, w1 = column_step(
            p_ref[i] - sound * d,
            w_ref[i] + BUOYANCY * heat_out[i],
            sound,
            inside,
            inverse,
        )
        d2_out[i] = d
        p1_out[i] = p1
        w2_out[i] = w1
    for i in range(rows):
        wide[i + 2, PAD : PAD + cols, :] = p1_out[i]
    for i in range(rows):
        d = d2_out[i] - bend(wide, i + 2, cols)
        p2, w2 = column_step(
            p1_out[i] - sound * d,
            w2_out[i] + BUOYANCY * heat_out[i],
            sound,
            inside,
            inverse,
        )
        d2_out[i] = d
        p2_out[i] = p2
        w2_out[i] = w2

    even_x, even_y = (even(axes[0]), even(axes[1]))
    for k, field in enumerate((p_ref, p1_out, p2_out)):
        for n in range(2):
            if k > 0:
                up, down = (field[rows - 2 + n], field[n])
                xa_out[2 * k + n] = jnp.where(even_x, up, down)
                xb_out[2 * k + n] = jnp.where(even_x, down, up)
            up, down = (field[:, cols - 2 + n, :], field[:, n, :])
            ya_out[2 * k + n] = jnp.where(even_y, up, down)
            yb_out[2 * k + n] = jnp.where(even_y, down, up)
    up, down = (p_ref[rows - 2] + 2.0 * u_ref[rows - 1], p_ref[1] - 2.0 * u_ref[0])
    xa_out[0] = jnp.where(even_x, up, p_ref[0])
    xa_out[1] = jnp.where(even_x, p_ref[rows - 1], down)
    xb_out[0] = jnp.where(even_x, p_ref[0], up)
    xb_out[1] = jnp.where(even_x, down, p_ref[rows - 1])
    up, down = (v_ref[:, cols - 1, :], v_ref[:, 0, :])
    ya_out[6] = jnp.where(even_y, up, down)
    yb_out[6] = jnp.where(even_y, down, up)
    for m, i in enumerate((0, rows - 1)):
        up, down = (u_ref[i, cols - 2 : cols, :], u_ref[i, 0:2, :])
        ya_out[7, 2 * m : 2 * m + 2, :] = jnp.where(even_y, up, down)
        yb_out[7, 2 * m : 2 * m + 2, :] = jnp.where(even_y, down, up)
    far_up, far_down = ([], [])
    for side, c in ((far_up, cols - 4), (far_down, 2)):
        for n in range(2):
            line = lambda ref, i: ref[i, c + n : c + n + 1, :]
            side += [line(p_ref, 0), line(p_ref, 1) - 2.0 * line(u_ref, 0)]
        for n in range(2):
            line = lambda ref, i: ref[i, c + n : c + n + 1, :]
            side += [
                line(p_ref, rows - 2) + 2.0 * line(u_ref, rows - 1),
                line(p_ref, rows - 1),
            ]
    up, down = (jnp.concatenate(far_up, axis=0), jnp.concatenate(far_down, axis=0))
    ya_out[8, 0:8, :] = jnp.where(even_y, up, down)
    yb_out[8, 0:8, :] = jnp.where(even_y, down, up)
    for out in (ya_out, yb_out):
        out[7, 4:, :] = jnp.zeros((rows - 4, levels), jnp.float32)
        out[9] = jnp.zeros((rows, levels), jnp.float32)
        out[9, 0:2, :] = sums_out[...]
    for m, i in enumerate((0, rows - 2)):
        for n in range(2):
            edge_out[4 * m + n : 4 * m + n + 1, :] = v_ref[i + n, 0:1, :]
            edge_out[4 * m + 2 + n : 4 * m + 3 + n, :] = v_ref[i + n, cols - 1 : cols, :]
    for m, i in enumerate((1, rows - 2)):
        edge_out[8 + 4 * m : 10 + 4 * m, :] = p_ref[i, 0:2, :]
        edge_out[10 + 4 * m : 12 + 4 * m, :] = p_ref[i, cols - 2 : cols, :]
    for step in range(steps):
        chunk_move(radius_out, radius_final, 2, step).wait()
    for move in moves[8:]:
        move.wait()


def first(sound, theta, humidity, radius_sq, multiplicity, count, p, u, v, w):
    slots = radius_sq.shape[0]
    rows, cols, levels = theta.shape
    hbm = pl.BlockSpec(memory_space=pltpu.HBM)
    f32 = lambda *shape: jax.ShapeDtypeStruct(shape, jnp.float32)
    block = f32(*theta.shape)
    outs = (
        [block, block, f32(*radius_sq.shape), f32(2, levels)]
        + [jax.ShapeDtypeStruct((2 * levels, 2 * levels), jnp.bfloat16)]
        + [block] * 5
        + [f32(6, cols, levels)] * 2
        + [f32(10, rows, levels)] * 2
        + [f32(16, levels)]
    )
    local_block = pltpu.VMEM(theta.shape, jnp.float32)
    layer_block = pltpu.VMEM(radius_sq.shape[1:], jnp.float32)
    return pl.pallas_call(
        functools.partial(first_kernel, ("gx", "gy")),
        in_specs=[hbm] * 10,
        out_specs=[hbm] * 3 + [VMEM] * 12,
        out_shape=outs,
        scratch_shapes=[
            layer_block,
            layer_block,
            pltpu.VMEM((levels, levels), jnp.float32),
            pltpu.VMEM((levels, levels), jnp.float32),
            pltpu.VMEM((rows + 4, cols + 2 * PAD, levels), jnp.float32),
            pltpu.VMEM(sound.shape, jnp.float32),
            local_block,
            local_block,
            pltpu.VMEM(radius_sq.shape, jnp.float32),
            pltpu.VMEM(multiplicity.shape, multiplicity.dtype),
            pltpu.VMEM(count.shape, count.dtype),
        ]
        + [local_block] * 5
        + [
            pltpu.VMEM(radius_sq.shape, jnp.float32),
            pltpu.SemaphoreType.DMA((10,)),
            pltpu.SemaphoreType.DMA((3, slots // CHUNK)),
        ],
        compiler_params=pltpu.CompilerParams(vmem_limit_bytes=GRANT),
        cost_estimate=pl.CostEstimate(
            flops=8_000_000_000, bytes_accessed=12_000_000, transcendentals=1_000_000
        ),
        name="condense_and_evolve",
    )(sound, theta, humidity, radius_sq, multiplicity, count, p, u, v, w)


def third_kernel(sound_ref, inverse_ref, heat_ref, p_ref, w_ref, d_ref, p_out, w_out, drift_out, wide):
    rows, cols, levels = p_ref.shape
    sound = sound_ref[...]
    inside = interior(levels)
    inverse = inverse_ref[...]
    clear_rim(wide, rows, cols)
    for i in range(rows):
        wide[i + 2, PAD : PAD + cols, :] = p_ref[i]
    for i in range(rows):
        d = d_ref[i] - bend(wide, i + 2, cols)
        p_out[i], w_out[i] = column_step(
            p_ref[i] - sound * d, w_ref[i] + BUOYANCY * heat_ref[i], sound, inside, inverse
        )
    r = lax.broadcasted_iota(jnp.int32, (levels, levels), 0)
    k = lax.broadcasted_iota(jnp.int32, (levels, levels), 1)
    push = jnp.where(k == r, -BUOYANCY, 0.0)
    drift_p, drift_w = (jnp.zeros_like(push), jnp.zeros_like(push))
    for _ in range(SUB):
        drift_p, drift_w = column_step(drift_p, drift_w + push, sound, inside, inverse)
    drift_out[:, 0:levels] = drift_p
    drift_out[:, levels:] = drift_w


def third(sound, weights, heat, p, w, d):
    rows, cols, levels = p.shape
    block = jax.ShapeDtypeStruct(p.shape, jnp.float32)
    return pl.pallas_call(
        third_kernel,
        in_specs=[VMEM] * 6,
        out_specs=[VMEM] * 3,
        out_shape=[block, block, jax.ShapeDtypeStruct((levels, 2 * levels), jnp.float32)],
        scratch_shapes=[pltpu.VMEM((rows + 4, cols + 2 * PAD, levels), jnp.float32)],
        compiler_params=pltpu.CompilerParams(vmem_limit_bytes=GRANT),
        cost_estimate=pl.CostEstimate(
            flops=2_000_000_000, bytes_accessed=4_000_000, transcendentals=0
        ),
        name="third_step",
    )(sound, weights, heat, p, w, d)


def corner_kernel(axes, ya_ref, yb_ref, edge_ref, sums_ref, a_out, b_out):
    even_x, even_y = (even(axes[0]), even(axes[1]))
    rows = ya_ref.shape[1]
    levels = ya_ref.shape[2]
    low = jnp.where(even_y, yb_ref[...], ya_ref[...])
    high = jnp.where(even_y, ya_ref[...], yb_ref[...])

    def put(at, up, down):
        size = up.shape[0]
        a_out[at : at + size, :] = jnp.where(even_x, up, down)
        b_out[at : at + size, :] = jnp.where(even_x, down, up)

    for m, side in enumerate((low, high)):
        at = SIDE * m
        for n in range(4):
            put(at + 2 * n, side[n, rows - 2 : rows], side[n, 0:2])
        put(at + 8, side[7, 2:4], side[7, 0:2])
        put(at + 10, side[6, rows - 2 : rows], side[6, 0:2])
        inner = (side[0] + 2.0 * side[6], side[1]) if m == 0 else (side[0], side[1] - 2.0 * side[6])
        for n in range(2):
            put(at + 12 + 2 * n, inner[n][rows - 4 : rows - 2], inner[n][2:4])
        put(at + 16, side[8, 4:8], side[8, 0:4])
    put(2 * SIDE, edge_ref[4:8, :], edge_ref[0:4, :])
    put(2 * SIDE + 4, edge_ref[12:16, :], edge_ref[8:12, :])
    both = sums_ref[...]
    put(2 * SIDE + 8, both, both)
    rest = jnp.zeros((EXTRA - 2 * SIDE - 10, levels), jnp.float32)
    put(2 * SIDE + 10, rest, rest)


def corner(ya, yb, edge, sums):
    levels = ya.shape[2]
    out = jax.ShapeDtypeStruct((EXTRA, levels), jnp.float32)
    return pl.pallas_call(
        functools.partial(corner_kernel, ("gx", "gy")),
        in_specs=[VMEM] * 4,
        out_specs=[VMEM] * 2,
        out_shape=[out, out],
        compiler_params=pltpu.CompilerParams(vmem_limit_bytes=GRANT),
        cost_estimate=pl.CostEstimate(flops=10_000_000, bytes_accessed=100_000, transcendentals=0),
        name="corner",
    )(ya, yb, edge, sums)


def cross(mu, field, rows, cols):
    for r in range(rows + 4):
        if r < 2 or rows <= r < rows + 2:
            mu[r] = 0.25 * field[r + 2]
        elif r < 4 or r >= rows + 2:
            mu[r] = 0.25 * field[r - 2]
        else:
            mu[r] = jnp.zeros(mu.shape[1:], jnp.float32)
    for c in range(2):
        for base in (PAD, PAD + cols):
            mu[:, base - 2 + c, :] += 0.25 * field[:, base + c, :]
            mu[:, base + c, :] += 0.25 * field[:, base - 2 + c, :]


def response_one(axes, sound_ref, inverse_ref, p0_ref, u_ref, v_ref, p1_ref, p2_ref, *refs):
    xa, xb, ya, yb, ca, cb, f0, f1, f2, yp, yw, yd, far_out, mu, urows, vcols = refs
    rows, cols, levels = p0_ref.shape
    ext = cols + 2 * PAD
    even_x, even_y = (even(axes[0]), even(axes[1]))
    sound = sound_ref[...]
    inside = interior(levels)
    inverse = inverse_ref[...]
    body = slice(PAD, PAD + cols)
    low_y = jnp.where(even_y, yb[...], ya[...])
    high_y = jnp.where(even_y, ya[...], yb[...])
    low_c = jnp.where(even_x, cb[...], ca[...])
    high_c = jnp.where(even_x, ca[...], cb[...])
    pick = lambda one, two, n: jnp.where(even_x, one[n], two[n])
    sides = ((low_y, PAD - 2), (high_y, PAD + cols))
    ends = ((low_c, 0, xb, xa), (high_c, rows + 2, xa, xb))

    for r in range(rows + 4):
        for f in (f0, f1, f2):
            f[r, 0:PAD, :] = jnp.zeros((PAD, levels), jnp.float32)
            f[r, PAD + cols :, :] = jnp.zeros((PAD, levels), jnp.float32)
    for k, (f, ref) in enumerate(((f0, p0_ref), (f1, p1_ref), (f2, p2_ref))):
        for i in range(rows):
            f[i + 2, body, :] = ref[i]
        for _, at, one, two in ends:
            for n in range(2):
                f[at + n, body, :] = pick(one, two, 2 * k + n)
        for side, at in sides:
            for n in range(2):
                f[2 : rows + 2, at + n, :] = side[2 * k + n]
        if k < 2:
            for corner_rows, at, _, _ in ends:
                for m, (_, c) in enumerate(sides):
                    for n in range(2):
                        start = SIDE * m + 4 * k + 2 * n
                        for e in range(2):
                            f[at + e, c + n : c + n + 1, :] = corner_rows[start + e : start + e + 1]
    virtual = []
    for m, (c_rows, at, one, two) in enumerate(ends):
        outer = at + m
        virtual.append(f0[outer, body, :])
        for n, c in enumerate((PAD, PAD + cols - 2)):
            start = 2 * SIDE + 4 + 2 * n
            f0[outer, c : c + 2, :] = c_rows[start : start + 2]
    urows[...] = jnp.zeros_like(urows)
    for m, (c_rows, at, one, two) in enumerate(ends):
        outer, inner = ((0, 1), (3, 2))[m]
        urows[inner, body, :] = u_ref[0 if m == 0 else rows - 1]
        for s, (side, c) in enumerate(sides):
            urows[outer, c : c + 2, :] = c_rows[SIDE * s + 8 : SIDE * s + 10]
            urows[inner, c : c + 2, :] = side[7, 2 * m : 2 * m + 2]
    for s, (side, c) in enumerate(sides):
        outer, inner = ((0, 1), (3, 2))[s]
        vcols[outer, 2 : rows + 2, :] = side[6]
        vcols[inner, 2 : rows + 2, :] = v_ref[:, 0 if s == 0 else cols - 1, :]
        for c_rows, at, _, _ in ends:
            vcols[outer, at : at + 2, :] = c_rows[SIDE * s + 10 : SIDE * s + 12]
            vcols[inner, at : at + 2, :] = c_rows[2 * SIDE + 2 * s : 2 * SIDE + 2 * s + 2]

    cross(mu, f0, rows, cols)
    mu[2, body, :] += 0.25 * (virtual[0] - f0[0, body, :])
    mu[rows + 1, body, :] += 0.25 * (virtual[1] - f0[rows + 3, body, :])
    mu[1] -= 0.5 * urows[1]
    mu[2] += 0.5 * urows[0]
    mu[rows + 1] -= 0.5 * urows[3]
    mu[rows + 2] += 0.5 * urows[2]
    mu[:, PAD - 1, :] -= 0.5 * vcols[1]
    mu[:, PAD, :] += 0.5 * vcols[0]
    mu[:, PAD + cols - 1, :] -= 0.5 * vcols[3]
    mu[:, PAD + cols, :] += 0.5 * vcols[2]
    for c_rows, row in ((low_c, 2), (high_c, rows)):
        for s, c in enumerate((PAD - 4, PAD + cols + 2)):
            for n in range(2):
                start = SIDE * s + 16 + 2 * n
                for e in range(2):
                    mu[row + e, c + n : c + n + 1, :] = 0.25 * c_rows[start + e : start + e + 1]
    far = 0.25 * jnp.concatenate(
        [c_rows[SIDE * s + 12 : SIDE * s + 16] for c_rows in (low_c, high_c) for s in range(2)],
        axis=0,
    )
    far, _ = column_step(sound * far, None, sound, inside, inverse)
    far_out[...] = 0.25 * far

    for r in range(rows + 4):
        if 4 <= r < rows:
            spans = (slice(0, 2 * PAD), slice(cols, ext))
            clear = jnp.zeros((cols - 2 * PAD, levels), jnp.float32)
            for y in (yp, yw, yd):
                y[r, 2 * PAD : cols, :] = clear
        else:
            spans = (slice(0, ext),)
        for span in spans:
            d = -mu[r, span, :]
            q = -sound * d
            yp[r, span, :], yw[r, span, :] = column_step(
                q, None, sound, inside, inverse
            )
            yd[r, span, :] = d


def response_two(shape, sound_ref, inverse_ref, f0, f1, f2, yp, yw, yd, far_ref, *refs):
    s_out, yp_out, yw_out, yd_out, mu = refs
    rows, cols, levels = shape
    ext = cols + 2 * PAD
    sound = sound_ref[...]
    inside = interior(levels)
    inverse = inverse_ref[...]
    cross(mu, f1, rows, cols)
    for r in range(rows + 4):
        y = yp[r]
        near = pltpu.roll(y, 2, 0) + pltpu.roll(y, ext - 2, 0)
        if r >= 2:
            near += yp[r - 2]
        if r < rows + 2:
            near += yp[r + 2]
        mu[r] += 0.25 * near - y
        s_out[r] = f0[r] + f1[r] + y
    for m, at in enumerate((0, rows + 2)):
        for s, c in enumerate((PAD, PAD + cols - 2)):
            for n in range(2):
                start = 8 * m + 4 * s + 2 * n
                for e in range(2):
                    mu[at + e, c + n : c + n + 1, :] += far_ref[start + e : start + e + 1, :]
    for r in range(rows + 4):
        d = yd[r] - mu[r]
        p, w = column_step(yp[r] - sound * d, yw[r], sound, inside, inverse)
        yd_out[r] = d
        yp_out[r] = p
        yw_out[r] = w
        s_out[r] += f2[r] + p


def response_three(columns, sound_ref, inverse_ref, u_ref, v_ref, p3_ref, w3_ref, f2, *refs):
    s_ref, yp, yw, yd, drift_ref, sums_ref = refs[:6]
    u_out, v_out, w_out, p_out, profile_out, mu = refs[6:]
    rows, cols, levels = u_ref.shape
    sound = sound_ref[...]
    inside = interior(levels)
    inverse = inverse_ref[...]
    body = slice(PAD, PAD + cols)
    cross(mu, f2, rows, cols)
    total = sums_ref[...] * (1.0 / columns)
    profile_out[...] = total[0:1]
    mean = jnp.broadcast_to(total[1:2], (8, levels))
    drift = exact_dot(mean, drift_ref[...])
    drift_p, drift_w = (drift[0:1, 0:levels], drift[0:1, levels:])
    for i in range(rows):
        r = i + 2
        d = yd[r, body, :] - mu[r, body, :] - bend(yp, r, cols)
        p, w = column_step(
            yp[r, body, :] - sound * d, yw[r, body, :], sound, inside, inverse
        )
        p_out[i] = p3_ref[i] + p + drift_p
        w_out[i] = w3_ref[i] + w + drift_w
        u_out[i] = u_ref[i] - 0.5 * (s_ref[r + 1, body, :] - s_ref[r - 1, body, :])
        east = lambda n: s_ref[r, PAD + n : PAD + n + cols, :]
        v_out[i] = v_ref[i] - 0.5 * (east(1) - east(-1))


def response(kernel, args, outs, scratch, flops):
    return pl.pallas_call(
        kernel,
        in_specs=[VMEM] * len(args),
        out_specs=[VMEM] * len(outs),
        out_shape=outs,
        scratch_shapes=scratch,
        compiler_params=pltpu.CompilerParams(vmem_limit_bytes=GRANT),
        cost_estimate=pl.CostEstimate(flops=flops, bytes_accessed=6_000_000, transcendentals=0),
    )(*args)


def swaps(count):
    near = [(i, i ^ 1) for i in range(count)]
    far = [(i, (i + 1) % count if i % 2 else (i - 1) % count) for i in range(count)]
    return near, far


def exchange(a, b, axis):
    near, far = swaps(lax.axis_size(axis))
    a = lax.ppermute(a, axis, near)
    b = lax.ppermute(b, axis, far)
    return a, b


def total_sum(value, axis):
    count = lax.axis_size(axis)
    distance = 2
    while distance < count:
        moved = lax.ppermute(value, axis, [(i, i ^ distance) for i in range(count)])
        value = value + moved
        distance *= 2
    return value


def window(
    eastward,
    northward,
    vertical,
    pressure,
    theta,
    humidity,
    sound_speed,
    radius_sq,
    multiplicity,
    droplet_count,
):
    columns = float(theta.shape[0] * theta.shape[1] * lax.axis_size("gx") * lax.axis_size("gy"))
    sound = sound_speed[None]
    (
        theta_out,
        humidity_out,
        radius_out,
        sums,
        weights,
        p1,
        p2,
        w2,
        d2,
        heat,
        xa,
        xb,
        ya,
        yb,
        edge,
    ) = first(
        *(
            pltpu.with_memory_space_constraint(x, pltpu.HBM)
            for x in (
                sound,
                theta,
                humidity,
                radius_sq,
                multiplicity,
                droplet_count,
                pressure,
                eastward,
                northward,
                vertical,
            )
        )
    )
    rows, cols, levels = theta.shape
    f32 = lambda *shape: jax.ShapeDtypeStruct(shape, jnp.float32)
    wide = (rows + 4, cols + 2 * PAD, levels)
    xa, xb = exchange(xa, xb, "gx")
    ya, yb = exchange(ya, yb, "gy")
    sums = total_sum(sums + ya[9, 0:2], "gy")
    ca, cb = corner(ya, yb, edge, sums)
    ca, cb = exchange(ca, cb, "gx")
    at = 2 * SIDE + 8
    sums = total_sum(sums + ca[at : at + 2], "gx")
    p3, w3, drift = third(sound, weights, heat, p2, w2, d2)
    f0, f1, f2, yp, yw, yd, far = response(
        functools.partial(response_one, ("gx", "gy")),
        (sound, weights, pressure, eastward, northward, p1, p2, xa, xb, ya, yb, ca, cb),
        [f32(*wide)] * 6 + [f32(16, levels)],
        [
            pltpu.VMEM(wide, jnp.float32),
            pltpu.VMEM((4, cols + 2 * PAD, levels), jnp.float32),
            pltpu.VMEM((4, rows + 4, levels), jnp.float32),
        ],
        4_000_000_000,
    )
    moved, yp, yw, yd = response(
        functools.partial(response_two, theta.shape),
        (sound, weights, f0, f1, f2, yp, yw, yd, far),
        [f32(*wide)] * 4,
        [pltpu.VMEM(wide, jnp.float32)],
        4_000_000_000,
    )
    u, v, w, p, profile = response(
        functools.partial(response_three, columns),
        (sound, weights, eastward, northward, p3, w3, f2, moved, yp, yw, yd, drift, sums),
        [f32(*theta.shape)] * 4 + [f32(1, levels)],
        [pltpu.VMEM(wide, jnp.float32)],
        2_000_000_000,
    )
    return (u, v, w, p, theta_out, humidity_out, radius_out, profile[0])


def solution(mesh):
    grid = P("gx", "gy", None)
    drops = P(None, None, "gx", "gy")
    return jax.shard_map(
        window,
        mesh=mesh,
        in_specs=(grid,) * 6 + (P(), drops, drops, P(None, "gx", "gy")),
        out_specs=(grid,) * 6 + (drops, P()),
        check_vma=False,
    )
```

```python
import functools

import jax
import jax.numpy as jnp
from jax import lax
from jax.experimental import pallas as pl
from jax.experimental.pallas import tpu as pltpu
from jax.sharding import PartitionSpec as P

SUB = 3
BUOYANCY = 0.5
VAPOUR_SLOPE = 0.01
GROWTH_RATE = 25.0
RADIUS_FLOOR = 0.0625
MASS_FACTOR = 0.0004
LATENT_HEAT = 200.0
TERMS = 6
CHUNK = 8
GRANT = 24 * 1024 * 1024
PAD = 8
SIDE = 20
EXTRA = 56

VMEM = pl.BlockSpec(memory_space=pltpu.VMEM)


def exact_dot(a, b):
    return jnp.dot(a, b, precision=lax.Precision.HIGHEST, preferred_element_type=jnp.float32)


def power15(x):
    return x * x * lax.rsqrt(x)


def split(x):
    high = x.astype(jnp.bfloat16)
    return high, (x - high.astype(jnp.float32)).astype(jnp.bfloat16)


def stack_weights(inverse, weights):
    levels = inverse.shape[0]
    high, low = split(inverse)
    weights[0:levels, 0:levels] = high
    weights[0:levels, levels:] = low
    weights[levels:, 0:levels] = high
    weights[levels:, levels:] = jnp.zeros_like(low)


def split_dot(x, weights):
    levels = x.shape[-1]
    both = jnp.concatenate(split(x), axis=1)
    out = jnp.dot(both, weights, preferred_element_type=jnp.float32)
    return out[:, :levels] + out[:, levels:]


def column_step(q, held, sound, inside, weights):
    levels = q.shape[-1]
    source = q - pltpu.roll(q, levels - 1, 1)
    if held is not None:
        source = source + held
    solved = split_dot(inside * source, weights)
    masked = solved * inside
    return (q - sound * (masked - pltpu.roll(masked, 1, 1)), solved)


def interior(levels):
    level = lax.broadcasted_iota(jnp.int32, (1, levels), 1)
    return (level < levels - 1).astype(jnp.float32)


def even(axis):
    return lax.rem(lax.axis_index(axis), 2) == 0


def clear_rim(wide, rows, cols):
    shape = wide.shape
    for r in (0, 1, rows + 2, rows + 3):
        wide[r] = jnp.zeros(shape[1:], jnp.float32)
    for r in range(2, rows + 2):
        wide[r, 0:PAD, :] = jnp.zeros((PAD, shape[2]), jnp.float32)
        wide[r, PAD + cols :, :] = jnp.zeros((PAD, shape[2]), jnp.float32)


def bend(wide, r, cols):
    east = lambda n: wide[r, PAD + n : PAD + n + cols, :]
    up = wide[r + 2, PAD : PAD + cols, :]
    down = wide[r - 2, PAD : PAD + cols, :]
    return 0.25 * ((up + down) + (east(2) + east(-2))) - east(0)


def inverse_start(sound, series, power):
    levels = series.shape[0]
    r = lax.broadcasted_iota(jnp.int32, (levels, levels), 0)
    k = lax.broadcasted_iota(jnp.int32, (levels, levels), 1)
    sound = jnp.broadcast_to(sound, (levels, levels))
    upper = jnp.where((k == r + 1) & (k < levels - 1), -sound, 0.0)
    above = pltpu.roll(sound, levels - 1, 1)
    diagonal = jnp.where(k == r, jnp.where(k < levels - 1, 1.0 + sound + above, 1.0), 0.0)
    eye = jnp.where(k == r, 1.0, 0.0)
    residual = eye - (diagonal + upper + upper.T) * (1.0 / 3.0)
    series[...] = eye * (1.0 / 3.0)
    power[...] = residual


def first_kernel(
    axes,
    sound_hbm,
    theta_hbm,
    humidity_hbm,
    radius_hbm,
    mult_hbm,
    count_hbm,
    p_hbm,
    u_hbm,
    v_hbm,
    w_hbm,
    theta_final,
    humidity_final,
    radius_final,
    sums_out,
    weights,
    p1_out,
    p2_out,
    w2_out,
    d2_out,
    heat_out,
    xa_out,
    xb_out,
    ya_out,
    yb_out,
    edge_out,
    cloud,
    total,
    power,
    series,
    wide,
    sound_ref,
    theta_ref,
    humidity_ref,
    radius_all,
    mult_all,
    count_ref,
    p_ref,
    u_ref,
    v_ref,
    w_ref,
    humidity_out,
    radius_out,
    sems,
    chunk_sems,
):
    steps = radius_all.shape[0] // CHUNK
    rows, cols, levels = theta_ref.shape
    layers = count_ref.shape[0]
    lowest = levels // 4
    pairs = (
        (theta_hbm, theta_ref),
        (humidity_hbm, humidity_ref),
        (sound_hbm, sound_ref),
        (count_hbm, count_ref),
        (p_hbm, p_ref),
        (u_hbm, u_ref),
        (v_hbm, v_ref),
        (w_hbm, w_ref),
        (heat_out, theta_final),
        (humidity_out, humidity_final),
    )
    moves = [pltpu.make_async_copy(x, y, sems.at[n]) for n, (x, y) in enumerate(pairs)]

    def chunk_move(x, y, kind, step):
        span = pl.ds(step * CHUNK, CHUNK)
        return pltpu.make_async_copy(x.at[span], y.at[span], chunk_sems.at[kind, step])

    for move in moves[:4]:
        move.start()
    for step in range(steps):
        chunk_move(radius_hbm, radius_all, 0, step).start()
        chunk_move(mult_hbm, mult_all, 1, step).start()
    for move in moves[4:8]:
        move.start()
    for move in moves[:4]:
        move.wait()
    for i in range(rows):
        sat = humidity_ref[i] * jnp.exp(-VAPOUR_SLOPE * theta_ref[i]) - 1.0
        cloud[:, i, :] = GROWTH_RATE * sat.T[lowest : lowest + layers]
    total[...] = jnp.zeros_like(total)
    inverse_start(sound_ref[...], series, power)
    assert steps >= TERMS

    @pl.loop(0, steps)
    def _(step):
        chunk_move(radius_hbm, radius_all, 0, step).wait()
        chunk_move(mult_hbm, mult_all, 1, step).wait()
        scale = power[...]
        series[...] += exact_dot(series[...], scale)
        power[...] = exact_dot(scale, scale)
        for n in range(CHUNK):
            s = step * CHUNK + n
            live = s < count_ref[...]
            radius = radius_all[s]
            grown = jnp.maximum(radius + cloud[...], RADIUS_FLOOR)
            radius_out[s] = jnp.where(live, grown, 0.0)
            mass = mult_all[s].astype(jnp.float32) * (power15(grown) - power15(radius))
            total[...] += jnp.where(live, mass, 0.0)
        chunk_move(radius_out, radius_final, 2, step).start()

    percent_sum = jnp.zeros((cols, levels), jnp.float32)
    theta_sum = jnp.zeros((cols, levels), jnp.float32)
    for i in range(rows):
        change = MASS_FACTOR * total[:, i, :]
        added = jnp.concatenate(
            [
                jnp.zeros((lowest, cols), jnp.float32),
                change,
                jnp.zeros((levels - lowest - layers, cols), jnp.float32),
            ],
            axis=0,
        ).T
        humid = humidity_ref[i] - added
        warm = theta_ref[i] + LATENT_HEAT * added
        humidity_out[i] = humid
        heat_out[i] = warm
        percent_sum += 100.0 * (humid * jnp.exp(-VAPOUR_SLOPE * warm) - 1.0)
        theta_sum += warm
    sums_out[0:1] = jnp.sum(percent_sum, axis=0, keepdims=True)
    sums_out[1:2] = jnp.sum(theta_sum, axis=0, keepdims=True)

    for move in moves[8:]:
        move.start()
    for move in moves[4:8]:
        move.wait()
    sound = sound_ref[...]
    inside = interior(levels)
    stack_weights(series[...], weights)
    inverse = weights[...]
    clear_rim(wide, rows, cols)
    for i in range(rows):
        wide[i + 2, PAD : PAD + cols, :] = p_ref[i]
    j = lax.broadcasted_iota(jnp.int32, (cols, levels), 0)
    for i in range(rows):
        spread = jnp.zeros((cols, levels), jnp.float32)
        if i + 1 < rows:
            spread += u_ref[i + 1]
        if i > 0:
            spread -= u_ref[i - 1]
        v = v_ref[i]
        spread += jnp.where(j < cols - 1, pltpu.roll(v, cols - 1, 0), 0.0)
        spread -= jnp.where(j > 0, pltpu.roll(v, 1, 0), 0.0)
        d = 0.5 * spread - bend(wide, i + 2, cols)
        p1, w1 = column_step(
            p_ref[i] - sound * d,
            w_ref[i] + BUOYANCY * heat_out[i],
            sound,
            inside,
            inverse,
        )
        d2_out[i] = d
        p1_out[i] = p1
        w2_out[i] = w1
    for i in range(rows):
        wide[i + 2, PAD : PAD + cols, :] = p1_out[i]
    for i in range(rows):
        d = d2_out[i] - bend(wide, i + 2, cols)
        p2, w2 = column_step(
            p1_out[i] - sound * d,
            w2_out[i] + BUOYANCY * heat_out[i],
            sound,
            inside,
            inverse,
        )
        d2_out[i] = d
        p2_out[i] = p2
        w2_out[i] = w2

    even_x, even_y = (even(axes[0]), even(axes[1]))
    for k, field in enumerate((p_ref, p1_out, p2_out)):
        for n in range(2):
            if k > 0:
                up, down = (field[rows - 2 + n], field[n])
                xa_out[2 * k + n] = jnp.where(even_x, up, down)
                xb_out[2 * k + n] = jnp.where(even_x, down, up)
            up, down = (field[:, cols - 2 + n, :], field[:, n, :])
            ya_out[2 * k + n] = jnp.where(even_y, up, down)
            yb_out[2 * k + n] = jnp.where(even_y, down, up)
    up, down = (p_ref[rows - 2] + 2.0 * u_ref[rows - 1], p_ref[1] - 2.0 * u_ref[0])
    xa_out[0] = jnp.where(even_x, up, p_ref[0])
    xa_out[1] = jnp.where(even_x, p_ref[rows - 1], down)
    xb_out[0] = jnp.where(even_x, p_ref[0], up)
    xb_out[1] = jnp.where(even_x, down, p_ref[rows - 1])
    up, down = (v_ref[:, cols - 1, :], v_ref[:, 0, :])
    ya_out[6] = jnp.where(even_y, up, down)
    yb_out[6] = jnp.where(even_y, down, up)
    for m, i in enumerate((0, rows - 1)):
        up, down = (u_ref[i, cols - 2 : cols, :], u_ref[i, 0:2, :])
        ya_out[7, 2 * m : 2 * m + 2, :] = jnp.where(even_y, up, down)
        yb_out[7, 2 * m : 2 * m + 2, :] = jnp.where(even_y, down, up)
    far_up, far_down = ([], [])
    for side, c in ((far_up, cols - 4), (far_down, 2)):
        for n in range(2):
            line = lambda ref, i: ref[i, c + n : c + n + 1, :]
            side += [line(p_ref, 0), line(p_ref, 1) - 2.0 * line(u_ref, 0)]
        for n in range(2):
            line = lambda ref, i: ref[i, c + n : c + n + 1, :]
            side += [
                line(p_ref, rows - 2) + 2.0 * line(u_ref, rows - 1),
                line(p_ref, rows - 1),
            ]
    up, down = (jnp.concatenate(far_up, axis=0), jnp.concatenate(far_down, axis=0))
    ya_out[8, 0:8, :] = jnp.where(even_y, up, down)
    yb_out[8, 0:8, :] = jnp.where(even_y, down, up)
    for out in (ya_out, yb_out):
        out[7, 4:, :] = jnp.zeros((rows - 4, levels), jnp.float32)
        out[9] = jnp.zeros((rows, levels), jnp.float32)
        out[9, 0:2, :] = sums_out[...]
    for m, i in enumerate((0, rows - 2)):
        for n in range(2):
            edge_out[4 * m + n : 4 * m + n + 1, :] = v_ref[i + n, 0:1, :]
            edge_out[4 * m + 2 + n : 4 * m + 3 + n, :] = v_ref[i + n, cols - 1 : cols, :]
    for m, i in enumerate((1, rows - 2)):
        edge_out[8 + 4 * m : 10 + 4 * m, :] = p_ref[i, 0:2, :]
        edge_out[10 + 4 * m : 12 + 4 * m, :] = p_ref[i, cols - 2 : cols, :]
    for step in range(steps):
        chunk_move(radius_out, radius_final, 2, step).wait()
    for move in moves[8:]:
        move.wait()


def first(sound, theta, humidity, radius_sq, multiplicity, count, p, u, v, w):
    slots = radius_sq.shape[0]
    rows, cols, levels = theta.shape
    hbm = pl.BlockSpec(memory_space=pltpu.HBM)
    f32 = lambda *shape: jax.ShapeDtypeStruct(shape, jnp.float32)
    block = f32(*theta.shape)
    outs = (
        [block, block, f32(*radius_sq.shape), f32(2, levels)]
        + [jax.ShapeDtypeStruct((2 * levels, 2 * levels), jnp.bfloat16)]
        + [block] * 5
        + [f32(6, cols, levels)] * 2
        + [f32(10, rows, levels)] * 2
        + [f32(16, levels)]
    )
    local_block = pltpu.VMEM(theta.shape, jnp.float32)
    layer_block = pltpu.VMEM(radius_sq.shape[1:], jnp.float32)
    return pl.pallas_call(
        functools.partial(first_kernel, ("gx", "gy")),
        in_specs=[hbm] * 10,
        out_specs=[hbm] * 3 + [VMEM] * 12,
        out_shape=outs,
        scratch_shapes=[
            layer_block,
            layer_block,
            pltpu.VMEM((levels, levels), jnp.float32),
            pltpu.VMEM((levels, levels), jnp.float32),
            pltpu.VMEM((rows + 4, cols + 2 * PAD, levels), jnp.float32),
            pltpu.VMEM(sound.shape, jnp.float32),
            local_block,
            local_block,
            pltpu.VMEM(radius_sq.shape, jnp.float32),
            pltpu.VMEM(multiplicity.shape, multiplicity.dtype),
            pltpu.VMEM(count.shape, count.dtype),
        ]
        + [local_block] * 5
        + [
            pltpu.VMEM(radius_sq.shape, jnp.float32),
            pltpu.SemaphoreType.DMA((10,)),
            pltpu.SemaphoreType.DMA((3, slots // CHUNK)),
        ],
        compiler_params=pltpu.CompilerParams(vmem_limit_bytes=GRANT),
        cost_estimate=pl.CostEstimate(
            flops=8_000_000_000, bytes_accessed=12_000_000, transcendentals=1_000_000
        ),
        name="condense_and_evolve",
    )(sound, theta, humidity, radius_sq, multiplicity, count, p, u, v, w)


def third_kernel(sound_ref, inverse_ref, heat_ref, p_ref, w_ref, d_ref, p_out, w_out, drift_out, wide):
    rows, cols, levels = p_ref.shape
    sound = sound_ref[...]
    inside = interior(levels)
    inverse = inverse_ref[...]
    clear_rim(wide, rows, cols)
    for i in range(rows):
        wide[i + 2, PAD : PAD + cols, :] = p_ref[i]
    for i in range(rows):
        d = d_ref[i] - bend(wide, i + 2, cols)
        p_out[i], w_out[i] = column_step(
            p_ref[i] - sound * d, w_ref[i] + BUOYANCY * heat_ref[i], sound, inside, inverse
        )
    r = lax.broadcasted_iota(jnp.int32, (levels, levels), 0)
    k = lax.broadcasted_iota(jnp.int32, (levels, levels), 1)
    push = jnp.where(k == r, -BUOYANCY, 0.0)
    drift_p, drift_w = (jnp.zeros_like(push), jnp.zeros_like(push))
    for _ in range(SUB):
        drift_p, drift_w = column_step(drift_p, drift_w + push, sound, inside, inverse)
    drift_out[:, 0:levels] = drift_p
    drift_out[:, levels:] = drift_w


def third(sound, weights, heat, p, w, d):
    rows, cols, levels = p.shape
    block = jax.ShapeDtypeStruct(p.shape, jnp.float32)
    return pl.pallas_call(
        third_kernel,
        in_specs=[VMEM] * 6,
        out_specs=[VMEM] * 3,
        out_shape=[block, block, jax.ShapeDtypeStruct((levels, 2 * levels), jnp.float32)],
        scratch_shapes=[pltpu.VMEM((rows + 4, cols + 2 * PAD, levels), jnp.float32)],
        compiler_params=pltpu.CompilerParams(vmem_limit_bytes=GRANT),
        cost_estimate=pl.CostEstimate(
            flops=2_000_000_000, bytes_accessed=4_000_000, transcendentals=0
        ),
        name="third_step",
    )(sound, weights, heat, p, w, d)


def corner_kernel(axes, ya_ref, yb_ref, edge_ref, sums_ref, a_out, b_out):
    even_x, even_y = (even(axes[0]), even(axes[1]))
    rows = ya_ref.shape[1]
    levels = ya_ref.shape[2]
    low = jnp.where(even_y, yb_ref[...], ya_ref[...])
    high = jnp.where(even_y, ya_ref[...], yb_ref[...])

    def put(at, up, down):
        size = up.shape[0]
        a_out[at : at + size, :] = jnp.where(even_x, up, down)
        b_out[at : at + size, :] = jnp.where(even_x, down, up)

    for m, side in enumerate((low, high)):
        at = SIDE * m
        for n in range(4):
            put(at + 2 * n, side[n, rows - 2 : rows], side[n, 0:2])
        put(at + 8, side[7, 2:4], side[7, 0:2])
        put(at + 10, side[6, rows - 2 : rows], side[6, 0:2])
        inner = (side[0] + 2.0 * side[6], side[1]) if m == 0 else (side[0], side[1] - 2.0 * side[6])
        for n in range(2):
            put(at + 12 + 2 * n, inner[n][rows - 4 : rows - 2], inner[n][2:4])
        put(at + 16, side[8, 4:8], side[8, 0:4])
    put(2 * SIDE, edge_ref[4:8, :], edge_ref[0:4, :])
    put(2 * SIDE + 4, edge_ref[12:16, :], edge_ref[8:12, :])
    both = sums_ref[...]
    put(2 * SIDE + 8, both, both)
    rest = jnp.zeros((EXTRA - 2 * SIDE - 10, levels), jnp.float32)
    put(2 * SIDE + 10, rest, rest)


def corner(ya, yb, edge, sums):
    levels = ya.shape[2]
    out = jax.ShapeDtypeStruct((EXTRA, levels), jnp.float32)
    return pl.pallas_call(
        functools.partial(corner_kernel, ("gx", "gy")),
        in_specs=[VMEM] * 4,
        out_specs=[VMEM] * 2,
        out_shape=[out, out],
        compiler_params=pltpu.CompilerParams(vmem_limit_bytes=GRANT),
        cost_estimate=pl.CostEstimate(flops=10_000_000, bytes_accessed=100_000, transcendentals=0),
        name="corner",
    )(ya, yb, edge, sums)


def cross(mu, field, rows, cols):
    for r in range(rows + 4):
        if r < 2 or rows <= r < rows + 2:
            mu[r] = 0.25 * field[r + 2]
        elif r < 4 or r >= rows + 2:
            mu[r] = 0.25 * field[r - 2]
        else:
            mu[r] = jnp.zeros(mu.shape[1:], jnp.float32)
    for c in range(2):
        for base in (PAD, PAD + cols):
            mu[:, base - 2 + c, :] += 0.25 * field[:, base + c, :]
            mu[:, base + c, :] += 0.25 * field[:, base - 2 + c, :]


def response_one(axes, sound_ref, inverse_ref, p0_ref, u_ref, v_ref, p1_ref, p2_ref, *refs):
    xa, xb, ya, yb, ca, cb, f0, f1, f2, yp, yw, yd, far_out, mu, urows, vcols = refs
    rows, cols, levels = p0_ref.shape
    ext = cols + 2 * PAD
    even_x, even_y = (even(axes[0]), even(axes[1]))
    sound = sound_ref[...]
    inside = interior(levels)
    inverse = inverse_ref[...]
    body = slice(PAD, PAD + cols)
    low_y = jnp.where(even_y, yb[...], ya[...])
    high_y = jnp.where(even_y, ya[...], yb[...])
    low_c = jnp.where(even_x, cb[...], ca[...])
    high_c = jnp.where(even_x, ca[...], cb[...])
    pick = lambda one, two, n: jnp.where(even_x, one[n], two[n])
    sides = ((low_y, PAD - 2), (high_y, PAD + cols))
    ends = ((low_c, 0, xb, xa), (high_c, rows + 2, xa, xb))

    for r in range(rows + 4):
        for f in (f0, f1, f2):
            f[r, 0:PAD, :] = jnp.zeros((PAD, levels), jnp.float32)
            f[r, PAD + cols :, :] = jnp.zeros((PAD, levels), jnp.float32)
    for k, (f, ref) in enumerate(((f0, p0_ref), (f1, p1_ref), (f2, p2_ref))):
        for i in range(rows):
            f[i + 2, body, :] = ref[i]
        for _, at, one, two in ends:
            for n in range(2):
                f[at + n, body, :] = pick(one, two, 2 * k + n)
        for side, at in sides:
            for n in range(2):
                f[2 : rows + 2, at + n, :] = side[2 * k + n]
        if k < 2:
            for corner_rows, at, _, _ in ends:
                for m, (_, c) in enumerate(sides):
                    for n in range(2):
                        start = SIDE * m + 4 * k + 2 * n
                        for e in range(2):
                            f[at + e, c + n : c + n + 1, :] = corner_rows[start + e : start + e + 1]
    virtual = []
    for m, (c_rows, at, one, two) in enumerate(ends):
        outer = at + m
        virtual.append(f0[outer, body, :])
        for n, c in enumerate((PAD, PAD + cols - 2)):
            start = 2 * SIDE + 4 + 2 * n
            f0[outer, c : c + 2, :] = c_rows[start : start + 2]
    urows[...] = jnp.zeros_like(urows)
    for m, (c_rows, at, one, two) in enumerate(ends):
        outer, inner = ((0, 1), (3, 2))[m]
        urows[inner, body, :] = u_ref[0 if m == 0 else rows - 1]
        for s, (side, c) in enumerate(sides):
            urows[outer, c : c + 2, :] = c_rows[SIDE * s + 8 : SIDE * s + 10]
            urows[inner, c : c + 2, :] = side[7, 2 * m : 2 * m + 2]
    for s, (side, c) in enumerate(sides):
        outer, inner = ((0, 1), (3, 2))[s]
        vcols[outer, 2 : rows + 2, :] = side[6]
        vcols[inner, 2 : rows + 2, :] = v_ref[:, 0 if s == 0 else cols - 1, :]
        for c_rows, at, _, _ in ends:
            vcols[outer, at : at + 2, :] = c_rows[SIDE * s + 10 : SIDE * s + 12]
            vcols[inner, at : at + 2, :] = c_rows[2 * SIDE + 2 * s : 2 * SIDE + 2 * s + 2]

    cross(mu, f0, rows, cols)
    mu[2, body, :] += 0.25 * (virtual[0] - f0[0, body, :])
    mu[rows + 1, body, :] += 0.25 * (virtual[1] - f0[rows + 3, body, :])
    mu[1] -= 0.5 * urows[1]
    mu[2] += 0.5 * urows[0]
    mu[rows + 1] -= 0.5 * urows[3]
    mu[rows + 2] += 0.5 * urows[2]
    mu[:, PAD - 1, :] -= 0.5 * vcols[1]
    mu[:, PAD, :] += 0.5 * vcols[0]
    mu[:, PAD + cols - 1, :] -= 0.5 * vcols[3]
    mu[:, PAD + cols, :] += 0.5 * vcols[2]
    for c_rows, row in ((low_c, 2), (high_c, rows)):
        for s, c in enumerate((PAD - 4, PAD + cols + 2)):
            for n in range(2):
                start = SIDE * s + 16 + 2 * n
                for e in range(2):
                    mu[row + e, c + n : c + n + 1, :] = 0.25 * c_rows[start + e : start + e + 1]
    far = 0.25 * jnp.concatenate(
        [c_rows[SIDE * s + 12 : SIDE * s + 16] for c_rows in (low_c, high_c) for s in range(2)],
        axis=0,
    )
    far, _ = column_step(sound * far, None, sound, inside, inverse)
    far_out[...] = 0.25 * far

    for r in range(rows + 4):
        if 4 <= r < rows:
            spans = (slice(0, 2 * PAD), slice(cols, ext))
            clear = jnp.zeros((cols - 2 * PAD, levels), jnp.float32)
            for y in (yp, yw, yd):
                y[r, 2 * PAD : cols, :] = clear
        else:
            spans = (slice(0, ext),)
        for span in spans:
            d = -mu[r, span, :]
            q = -sound * d
            yp[r, span, :], yw[r, span, :] = column_step(
                q, None, sound, inside, inverse
            )
            yd[r, span, :] = d


def response_two(shape, sound_ref, inverse_ref, f0, f1, f2, yp, yw, yd, far_ref, *refs):
    s_out, yp_out, yw_out, yd_out, mu = refs
    rows, cols, levels = shape
    ext = cols + 2 * PAD
    sound = sound_ref[...]
    inside = interior(levels)
    inverse = inverse_ref[...]
    cross(mu, f1, rows, cols)
    for r in range(rows + 4):
        y = yp[r]
        near = pltpu.roll(y, 2, 0) + pltpu.roll(y, ext - 2, 0)
        if r >= 2:
            near += yp[r - 2]
        if r < rows + 2:
            near += yp[r + 2]
        mu[r] += 0.25 * near - y
        s_out[r] = f0[r] + f1[r] + y
    for m, at in enumerate((0, rows + 2)):
        for s, c in enumerate((PAD, PAD + cols - 2)):
            for n in range(2):
                start = 8 * m + 4 * s + 2 * n
                for e in range(2):
                    mu[at + e, c + n : c + n + 1, :] += far_ref[start + e : start + e + 1, :]
    for r in range(rows + 4):
        d = yd[r] - mu[r]
        p, w = column_step(yp[r] - sound * d, yw[r], sound, inside, inverse)
        yd_out[r] = d
        yp_out[r] = p
        yw_out[r] = w
        s_out[r] += f2[r] + p


def response_three(sound_ref, inverse_ref, u_ref, v_ref, p3_ref, w3_ref, f2, *refs):
    s_ref, yp, yw, yd, u_out, v_out, w_out, p_out, mu = refs
    rows, cols, levels = u_ref.shape
    sound = sound_ref[...]
    inside = interior(levels)
    inverse = inverse_ref[...]
    body = slice(PAD, PAD + cols)
    cross(mu, f2, rows, cols)
    for i in range(rows):
        r = i + 2
        d = yd[r, body, :] - mu[r, body, :] - bend(yp, r, cols)
        p, w = column_step(
            yp[r, body, :] - sound * d, yw[r, body, :], sound, inside, inverse
        )
        p_out[i] = p3_ref[i] + p
        w_out[i] = w3_ref[i] + w
        u_out[i] = u_ref[i] - 0.5 * (s_ref[r + 1, body, :] - s_ref[r - 1, body, :])
        east = lambda n: s_ref[r, PAD + n : PAD + n + cols, :]
        v_out[i] = v_ref[i] - 0.5 * (east(1) - east(-1))


def settle_kernel(columns, p_ref, w_ref, drift_ref, sums_ref, w_out, p_out, profile_out):
    rows, _, levels = p_ref.shape
    total = sums_ref[...] * (1.0 / columns)
    profile_out[...] = total[0:1]
    mean = jnp.broadcast_to(total[1:2], (8, levels))
    drift = exact_dot(mean, drift_ref[...])
    for i in range(rows):
        p_out[i] = p_ref[i] + drift[0:1, 0:levels]
        w_out[i] = w_ref[i] + drift[0:1, levels:]


def response(kernel, args, outs, scratch, flops):
    return pl.pallas_call(
        kernel,
        in_specs=[VMEM] * len(args),
        out_specs=[VMEM] * len(outs),
        out_shape=outs,
        scratch_shapes=scratch,
        compiler_params=pltpu.CompilerParams(vmem_limit_bytes=GRANT),
        cost_estimate=pl.CostEstimate(flops=flops, bytes_accessed=6_000_000, transcendentals=0),
    )(*args)


def swaps(count):
    near = [(i, i ^ 1) for i in range(count)]
    far = [(i, (i + 1) % count if i % 2 else (i - 1) % count) for i in range(count)]
    return near, far


def exchange(a, b, axis):
    near, far = swaps(lax.axis_size(axis))
    a = lax.ppermute(a, axis, near)
    b = lax.ppermute(b, axis, far)
    return a, b


def total_sum(value, axis):
    count = lax.axis_size(axis)
    distance = 2
    while distance < count:
        moved = lax.ppermute(value, axis, [(i, i ^ distance) for i in range(count)])
        value = value + moved
        distance *= 2
    return value


def window(
    eastward,
    northward,
    vertical,
    pressure,
    theta,
    humidity,
    sound_speed,
    radius_sq,
    multiplicity,
    droplet_count,
):
    columns = float(theta.shape[0] * theta.shape[1] * lax.axis_size("gx") * lax.axis_size("gy"))
    sound = sound_speed[None]
    (
        theta_out,
        humidity_out,
        radius_out,
        sums,
        weights,
        p1,
        p2,
        w2,
        d2,
        heat,
        xa,
        xb,
        ya,
        yb,
        edge,
    ) = first(
        *(
            pltpu.with_memory_space_constraint(x, pltpu.HBM)
            for x in (
                sound,
                theta,
                humidity,
                radius_sq,
                multiplicity,
                droplet_count,
                pressure,
                eastward,
                northward,
                vertical,
            )
        )
    )
    rows, cols, levels = theta.shape
    f32 = lambda *shape: jax.ShapeDtypeStruct(shape, jnp.float32)
    wide = (rows + 4, cols + 2 * PAD, levels)
    xa, xb = exchange(xa, xb, "gx")
    ya, yb = exchange(ya, yb, "gy")
    sums = total_sum(sums + ya[9, 0:2], "gy")
    ca, cb = corner(ya, yb, edge, sums)
    ca, cb = exchange(ca, cb, "gx")
    at = 2 * SIDE + 8
    sums = total_sum(sums + ca[at : at + 2], "gx")
    p3, w3, drift = third(sound, weights, heat, p2, w2, d2)
    f0, f1, f2, yp, yw, yd, far = response(
        functools.partial(response_one, ("gx", "gy")),
        (sound, weights, pressure, eastward, northward, p1, p2, xa, xb, ya, yb, ca, cb),
        [f32(*wide)] * 6 + [f32(16, levels)],
        [
            pltpu.VMEM(wide, jnp.float32),
            pltpu.VMEM((4, cols + 2 * PAD, levels), jnp.float32),
            pltpu.VMEM((4, rows + 4, levels), jnp.float32),
        ],
        4_000_000_000,
    )
    moved, yp, yw, yd = response(
        functools.partial(response_two, theta.shape),
        (sound, weights, f0, f1, f2, yp, yw, yd, far),
        [f32(*wide)] * 4,
        [pltpu.VMEM(wide, jnp.float32)],
        4_000_000_000,
    )
    u, v, w, p = response(
        response_three,
        (sound, weights, eastward, northward, p3, w3, f2, moved, yp, yw, yd),
        [f32(*theta.shape)] * 4,
        [pltpu.VMEM(wide, jnp.float32)],
        4_000_000_000,
    )
    w, p, profile = response(
        functools.partial(settle_kernel, columns),
        (p, w, drift, sums),
        [f32(*theta.shape)] * 2 + [f32(1, levels)],
        [],
        100_000_000,
    )
    return (u, v, w, p, theta_out, humidity_out, radius_out, profile[0])


def solution(mesh):
    grid = P("gx", "gy", None)
    drops = P(None, None, "gx", "gy")
    return jax.shard_map(
        window,
        mesh=mesh,
        in_specs=(grid,) * 6 + (P(), drops, drops, P(None, "gx", "gy")),
        out_specs=(grid,) * 6 + (drops, P()),
        check_vma=False,
    )
```

```python
import functools

import jax
import jax.numpy as jnp
from jax import lax
from jax.experimental import pallas as pl
from jax.experimental.pallas import tpu as pltpu
from jax.sharding import PartitionSpec as P

SUB = 3
BUOYANCY = 0.5
VAPOUR_SLOPE = 0.01
GROWTH_RATE = 25.0
RADIUS_FLOOR = 0.0625
MASS_FACTOR = 0.0004
LATENT_HEAT = 200.0
TERMS = 6
CHUNK = 8
GRANT = 24 * 1024 * 1024
PAD = 8
SIDE = 20
EXTRA = 56

VMEM = pl.BlockSpec(memory_space=pltpu.VMEM)


def exact_dot(a, b):
    return jnp.dot(a, b, precision=lax.Precision.HIGHEST, preferred_element_type=jnp.float32)


def power15(x):
    return x * x * lax.rsqrt(x)


def split(x):
    high = x.astype(jnp.bfloat16)
    return high, (x - high.astype(jnp.float32)).astype(jnp.bfloat16)


def stack_weights(inverse, weights):
    levels = inverse.shape[0]
    high, low = split(inverse)
    weights[0:levels, 0:levels] = high
    weights[0:levels, levels:] = low
    weights[levels:, 0:levels] = high
    weights[levels:, levels:] = jnp.zeros_like(low)


def split_dot(x, weights):
    levels = x.shape[-1]
    both = jnp.concatenate(split(x), axis=1)
    out = jnp.dot(both, weights, preferred_element_type=jnp.float32)
    return out[:, :levels] + out[:, levels:]


def column_step(q, held, sound, inside, weights):
    levels = q.shape[-1]
    source = q - pltpu.roll(q, levels - 1, 1)
    if held is not None:
        source = source + held
    solved = split_dot(inside * source, weights)
    masked = solved * inside
    return (q - sound * (masked - pltpu.roll(masked, 1, 1)), solved)


def interior(levels):
    level = lax.broadcasted_iota(jnp.int32, (1, levels), 1)
    return (level < levels - 1).astype(jnp.float32)


def even(axis):
    return lax.rem(lax.axis_index(axis), 2) == 0


def clear_rim(wide, rows, cols):
    shape = wide.shape
    for r in (0, 1, rows + 2, rows + 3):
        wide[r] = jnp.zeros(shape[1:], jnp.float32)
    for r in range(2, rows + 2):
        wide[r, 0:PAD, :] = jnp.zeros((PAD, shape[2]), jnp.float32)
        wide[r, PAD + cols :, :] = jnp.zeros((PAD, shape[2]), jnp.float32)


def bend(wide, r, cols):
    east = lambda n: wide[r, PAD + n : PAD + n + cols, :]
    up = wide[r + 2, PAD : PAD + cols, :]
    down = wide[r - 2, PAD : PAD + cols, :]
    return 0.25 * ((up + down) + (east(2) + east(-2))) - east(0)


def inverse_start(sound, series, power):
    levels = series.shape[0]
    r = lax.broadcasted_iota(jnp.int32, (levels, levels), 0)
    k = lax.broadcasted_iota(jnp.int32, (levels, levels), 1)
    sound = jnp.broadcast_to(sound, (levels, levels))
    upper = jnp.where((k == r + 1) & (k < levels - 1), -sound, 0.0)
    above = pltpu.roll(sound, levels - 1, 1)
    diagonal = jnp.where(k == r, jnp.where(k < levels - 1, 1.0 + sound + above, 1.0), 0.0)
    eye = jnp.where(k == r, 1.0, 0.0)
    residual = eye - (diagonal + upper + upper.T) * (1.0 / 3.0)
    series[...] = eye * (1.0 / 3.0)
    power[...] = residual


def first_kernel(
    axes,
    sound_hbm,
    theta_hbm,
    humidity_hbm,
    radius_hbm,
    mult_hbm,
    count_hbm,
    p_hbm,
    u_hbm,
    v_hbm,
    w_hbm,
    theta_final,
    humidity_final,
    radius_final,
    sums_out,
    weights,
    p1_out,
    p2_out,
    w2_out,
    d2_out,
    heat_out,
    xa_out,
    xb_out,
    ya_out,
    yb_out,
    edge_out,
    cloud,
    total,
    power,
    series,
    wide,
    sound_ref,
    theta_ref,
    humidity_ref,
    radius_all,
    mult_all,
    count_ref,
    p_ref,
    u_ref,
    v_ref,
    w_ref,
    humidity_out,
    radius_out,
    sems,
    chunk_sems,
):
    steps = radius_all.shape[0] // CHUNK
    rows, cols, levels = theta_ref.shape
    layers = count_ref.shape[0]
    lowest = levels // 4
    pairs = (
        (theta_hbm, theta_ref),
        (humidity_hbm, humidity_ref),
        (sound_hbm, sound_ref),
        (count_hbm, count_ref),
        (p_hbm, p_ref),
        (u_hbm, u_ref),
        (v_hbm, v_ref),
        (w_hbm, w_ref),
        (heat_out, theta_final),
        (humidity_out, humidity_final),
    )
    moves = [pltpu.make_async_copy(x, y, sems.at[n]) for n, (x, y) in enumerate(pairs)]

    def chunk_move(x, y, kind, step):
        span = pl.ds(step * CHUNK, CHUNK)
        return pltpu.make_async_copy(x.at[span], y.at[span], chunk_sems.at[kind, step])

    for move in moves[:4]:
        move.start()
    chunk_move(radius_hbm, radius_all, 0, 0).start()
    chunk_move(mult_hbm, mult_all, 1, 0).start()
    for move in moves[:4]:
        move.wait()
    for step in range(1, steps):
        chunk_move(radius_hbm, radius_all, 0, step).start()
        chunk_move(mult_hbm, mult_all, 1, step).start()
    for move in moves[4:8]:
        move.start()
    for i in range(rows):
        sat = humidity_ref[i] * jnp.exp(-VAPOUR_SLOPE * theta_ref[i]) - 1.0
        cloud[:, i, :] = GROWTH_RATE * sat.T[lowest : lowest + layers]
    total[...] = jnp.zeros_like(total)
    inverse_start(sound_ref[...], series, power)
    assert steps >= TERMS

    @pl.loop(0, steps)
    def _(step):
        chunk_move(radius_hbm, radius_all, 0, step).wait()
        chunk_move(mult_hbm, mult_all, 1, step).wait()
        scale = power[...]
        series[...] += exact_dot(series[...], scale)
        power[...] = exact_dot(scale, scale)
        for n in range(CHUNK):
            s = step * CHUNK + n
            live = s < count_ref[...]
            radius = radius_all[s]
            grown = jnp.maximum(radius + cloud[...], RADIUS_FLOOR)
            radius_out[s] = jnp.where(live, grown, 0.0)
            mass = mult_all[s].astype(jnp.float32) * (power15(grown) - power15(radius))
            total[...] += jnp.where(live, mass, 0.0)
        chunk_move(radius_out, radius_final, 2, step).start()

    percent_sum = jnp.zeros((cols, levels), jnp.float32)
    theta_sum = jnp.zeros((cols, levels), jnp.float32)
    for i in range(rows):
        change = MASS_FACTOR * total[:, i, :]
        added = jnp.concatenate(
            [
                jnp.zeros((lowest, cols), jnp.float32),
                change,
                jnp.zeros((levels - lowest - layers, cols), jnp.float32),
            ],
            axis=0,
        ).T
        humid = humidity_ref[i] - added
        warm = theta_ref[i] + LATENT_HEAT * added
        humidity_out[i] = humid
        heat_out[i] = warm
        percent_sum += 100.0 * (humid * jnp.exp(-VAPOUR_SLOPE * warm) - 1.0)
        theta_sum += warm
    sums_out[0:1] = jnp.sum(percent_sum, axis=0, keepdims=True)
    sums_out[1:2] = jnp.sum(theta_sum, axis=0, keepdims=True)

    for move in moves[8:]:
        move.start()
    for move in moves[4:8]:
        move.wait()
    sound = sound_ref[...]
    inside = interior(levels)
    stack_weights(series[...], weights)
    inverse = weights[...]
    clear_rim(wide, rows, cols)
    for i in range(rows):
        wide[i + 2, PAD : PAD + cols, :] = p_ref[i]
    j = lax.broadcasted_iota(jnp.int32, (cols, levels), 0)
    for i in range(rows):
        spread = jnp.zeros((cols, levels), jnp.float32)
        if i + 1 < rows:
            spread += u_ref[i + 1]
        if i > 0:
            spread -= u_ref[i - 1]
        v = v_ref[i]
        spread += jnp.where(j < cols - 1, pltpu.roll(v, cols - 1, 0), 0.0)
        spread -= jnp.where(j > 0, pltpu.roll(v, 1, 0), 0.0)
        d = 0.5 * spread - bend(wide, i + 2, cols)
        p1, w1 = column_step(
            p_ref[i] - sound * d,
            w_ref[i] + BUOYANCY * heat_out[i],
            sound,
            inside,
            inverse,
        )
        d2_out[i] = d
        p1_out[i] = p1
        w2_out[i] = w1
    for i in range(rows):
        wide[i + 2, PAD : PAD + cols, :] = p1_out[i]
    for i in range(rows):
        d = d2_out[i] - bend(wide, i + 2, cols)
        p2, w2 = column_step(
            p1_out[i] - sound * d,
            w2_out[i] + BUOYANCY * heat_out[i],
            sound,
            inside,
            inverse,
        )
        d2_out[i] = d
        p2_out[i] = p2
        w2_out[i] = w2

    even_x, even_y = (even(axes[0]), even(axes[1]))
    for k, field in enumerate((p_ref, p1_out, p2_out)):
        for n in range(2):
            if k > 0:
                up, down = (field[rows - 2 + n], field[n])
                xa_out[2 * k + n] = jnp.where(even_x, up, down)
                xb_out[2 * k + n] = jnp.where(even_x, down, up)
            up, down = (field[:, cols - 2 + n, :], field[:, n, :])
            ya_out[2 * k + n] = jnp.where(even_y, up, down)
            yb_out[2 * k + n] = jnp.where(even_y, down, up)
    up, down = (p_ref[rows - 2] + 2.0 * u_ref[rows - 1], p_ref[1] - 2.0 * u_ref[0])
    xa_out[0] = jnp.where(even_x, up, p_ref[0])
    xa_out[1] = jnp.where(even_x, p_ref[rows - 1], down)
    xb_out[0] = jnp.where(even_x, p_ref[0], up)
    xb_out[1] = jnp.where(even_x, down, p_ref[rows - 1])
    up, down = (v_ref[:, cols - 1, :], v_ref[:, 0, :])
    ya_out[6] = jnp.where(even_y, up, down)
    yb_out[6] = jnp.where(even_y, down, up)
    for m, i in enumerate((0, rows - 1)):
        up, down = (u_ref[i, cols - 2 : cols, :], u_ref[i, 0:2, :])
        ya_out[7, 2 * m : 2 * m + 2, :] = jnp.where(even_y, up, down)
        yb_out[7, 2 * m : 2 * m + 2, :] = jnp.where(even_y, down, up)
    far_up, far_down = ([], [])
    for side, c in ((far_up, cols - 4), (far_down, 2)):
        for n in range(2):
            line = lambda ref, i: ref[i, c + n : c + n + 1, :]
            side += [line(p_ref, 0), line(p_ref, 1) - 2.0 * line(u_ref, 0)]
        for n in range(2):
            line = lambda ref, i: ref[i, c + n : c + n + 1, :]
            side += [
                line(p_ref, rows - 2) + 2.0 * line(u_ref, rows - 1),
                line(p_ref, rows - 1),
            ]
    up, down = (jnp.concatenate(far_up, axis=0), jnp.concatenate(far_down, axis=0))
    ya_out[8, 0:8, :] = jnp.where(even_y, up, down)
    yb_out[8, 0:8, :] = jnp.where(even_y, down, up)
    for out in (ya_out, yb_out):
        out[7, 4:, :] = jnp.zeros((rows - 4, levels), jnp.float32)
        out[9] = jnp.zeros((rows, levels), jnp.float32)
        out[9, 0:2, :] = sums_out[...]
    for m, i in enumerate((0, rows - 2)):
        for n in range(2):
            edge_out[4 * m + n : 4 * m + n + 1, :] = v_ref[i + n, 0:1, :]
            edge_out[4 * m + 2 + n : 4 * m + 3 + n, :] = v_ref[i + n, cols - 1 : cols, :]
    for m, i in enumerate((1, rows - 2)):
        edge_out[8 + 4 * m : 10 + 4 * m, :] = p_ref[i, 0:2, :]
        edge_out[10 + 4 * m : 12 + 4 * m, :] = p_ref[i, cols - 2 : cols, :]
    for step in range(steps):
        chunk_move(radius_out, radius_final, 2, step).wait()
    for move in moves[8:]:
        move.wait()


def first(sound, theta, humidity, radius_sq, multiplicity, count, p, u, v, w):
    slots = radius_sq.shape[0]
    rows, cols, levels = theta.shape
    hbm = pl.BlockSpec(memory_space=pltpu.HBM)
    f32 = lambda *shape: jax.ShapeDtypeStruct(shape, jnp.float32)
    block = f32(*theta.shape)
    outs = (
        [block, block, f32(*radius_sq.shape), f32(2, levels)]
        + [jax.ShapeDtypeStruct((2 * levels, 2 * levels), jnp.bfloat16)]
        + [block] * 5
        + [f32(6, cols, levels)] * 2
        + [f32(10, rows, levels)] * 2
        + [f32(16, levels)]
    )
    local_block = pltpu.VMEM(theta.shape, jnp.float32)
    layer_block = pltpu.VMEM(radius_sq.shape[1:], jnp.float32)
    return pl.pallas_call(
        functools.partial(first_kernel, ("gx", "gy")),
        in_specs=[hbm] * 10,
        out_specs=[hbm] * 3 + [VMEM] * 12,
        out_shape=outs,
        scratch_shapes=[
            layer_block,
            layer_block,
            pltpu.VMEM((levels, levels), jnp.float32),
            pltpu.VMEM((levels, levels), jnp.float32),
            pltpu.VMEM((rows + 4, cols + 2 * PAD, levels), jnp.float32),
            pltpu.VMEM(sound.shape, jnp.float32),
            local_block,
            local_block,
            pltpu.VMEM(radius_sq.shape, jnp.float32),
            pltpu.VMEM(multiplicity.shape, multiplicity.dtype),
            pltpu.VMEM(count.shape, count.dtype),
        ]
        + [local_block] * 5
        + [
            pltpu.VMEM(radius_sq.shape, jnp.float32),
            pltpu.SemaphoreType.DMA((10,)),
            pltpu.SemaphoreType.DMA((3, slots // CHUNK)),
        ],
        compiler_params=pltpu.CompilerParams(vmem_limit_bytes=GRANT),
        cost_estimate=pl.CostEstimate(
            flops=8_000_000_000, bytes_accessed=12_000_000, transcendentals=1_000_000
        ),
        name="condense_and_evolve",
    )(sound, theta, humidity, radius_sq, multiplicity, count, p, u, v, w)


def third_kernel(sound_ref, inverse_ref, heat_ref, p_ref, w_ref, d_ref, p_out, w_out, drift_out, wide):
    rows, cols, levels = p_ref.shape
    sound = sound_ref[...]
    inside = interior(levels)
    inverse = inverse_ref[...]
    clear_rim(wide, rows, cols)
    for i in range(rows):
        wide[i + 2, PAD : PAD + cols, :] = p_ref[i]
    for i in range(rows):
        d = d_ref[i] - bend(wide, i + 2, cols)
        p_out[i], w_out[i] = column_step(
            p_ref[i] - sound * d, w_ref[i] + BUOYANCY * heat_ref[i], sound, inside, inverse
        )
    r = lax.broadcasted_iota(jnp.int32, (levels, levels), 0)
    k = lax.broadcasted_iota(jnp.int32, (levels, levels), 1)
    push = jnp.where(k == r, -BUOYANCY, 0.0)
    drift_p, drift_w = (jnp.zeros_like(push), jnp.zeros_like(push))
    for _ in range(SUB):
        drift_p, drift_w = column_step(drift_p, drift_w + push, sound, inside, inverse)
    drift_out[:, 0:levels] = drift_p
    drift_out[:, levels:] = drift_w


def third(sound, weights, heat, p, w, d):
    rows, cols, levels = p.shape
    block = jax.ShapeDtypeStruct(p.shape, jnp.float32)
    return pl.pallas_call(
        third_kernel,
        in_specs=[VMEM] * 6,
        out_specs=[VMEM] * 3,
        out_shape=[block, block, jax.ShapeDtypeStruct((levels, 2 * levels), jnp.float32)],
        scratch_shapes=[pltpu.VMEM((rows + 4, cols + 2 * PAD, levels), jnp.float32)],
        compiler_params=pltpu.CompilerParams(vmem_limit_bytes=GRANT),
        cost_estimate=pl.CostEstimate(
            flops=2_000_000_000, bytes_accessed=4_000_000, transcendentals=0
        ),
        name="third_step",
    )(sound, weights, heat, p, w, d)


def corner_kernel(axes, ya_ref, yb_ref, edge_ref, sums_ref, a_out, b_out):
    even_x, even_y = (even(axes[0]), even(axes[1]))
    rows = ya_ref.shape[1]
    levels = ya_ref.shape[2]
    low = jnp.where(even_y, yb_ref[...], ya_ref[...])
    high = jnp.where(even_y, ya_ref[...], yb_ref[...])

    def put(at, up, down):
        size = up.shape[0]
        a_out[at : at + size, :] = jnp.where(even_x, up, down)
        b_out[at : at + size, :] = jnp.where(even_x, down, up)

    for m, side in enumerate((low, high)):
        at = SIDE * m
        for n in range(4):
            put(at + 2 * n, side[n, rows - 2 : rows], side[n, 0:2])
        put(at + 8, side[7, 2:4], side[7, 0:2])
        put(at + 10, side[6, rows - 2 : rows], side[6, 0:2])
        inner = (side[0] + 2.0 * side[6], side[1]) if m == 0 else (side[0], side[1] - 2.0 * side[6])
        for n in range(2):
            put(at + 12 + 2 * n, inner[n][rows - 4 : rows - 2], inner[n][2:4])
        put(at + 16, side[8, 4:8], side[8, 0:4])
    put(2 * SIDE, edge_ref[4:8, :], edge_ref[0:4, :])
    put(2 * SIDE + 4, edge_ref[12:16, :], edge_ref[8:12, :])
    both = sums_ref[...]
    put(2 * SIDE + 8, both, both)
    rest = jnp.zeros((EXTRA - 2 * SIDE - 10, levels), jnp.float32)
    put(2 * SIDE + 10, rest, rest)


def corner(ya, yb, edge, sums):
    levels = ya.shape[2]
    out = jax.ShapeDtypeStruct((EXTRA, levels), jnp.float32)
    return pl.pallas_call(
        functools.partial(corner_kernel, ("gx", "gy")),
        in_specs=[VMEM] * 4,
        out_specs=[VMEM] * 2,
        out_shape=[out, out],
        compiler_params=pltpu.CompilerParams(vmem_limit_bytes=GRANT),
        cost_estimate=pl.CostEstimate(flops=10_000_000, bytes_accessed=100_000, transcendentals=0),
        name="corner",
    )(ya, yb, edge, sums)


def cross(mu, field, rows, cols):
    for r in range(rows + 4):
        if r < 2 or rows <= r < rows + 2:
            mu[r] = 0.25 * field[r + 2]
        elif r < 4 or r >= rows + 2:
            mu[r] = 0.25 * field[r - 2]
        else:
            mu[r] = jnp.zeros(mu.shape[1:], jnp.float32)
    for c in range(2):
        for base in (PAD, PAD + cols):
            mu[:, base - 2 + c, :] += 0.25 * field[:, base + c, :]
            mu[:, base + c, :] += 0.25 * field[:, base - 2 + c, :]


def response_one(axes, sound_ref, inverse_ref, p0_ref, u_ref, v_ref, p1_ref, p2_ref, *refs):
    xa, xb, ya, yb, ca, cb, f0, f1, f2, yp, yw, yd, far_out, mu, urows, vcols = refs
    rows, cols, levels = p0_ref.shape
    ext = cols + 2 * PAD
    even_x, even_y = (even(axes[0]), even(axes[1]))
    sound = sound_ref[...]
    inside = interior(levels)
    inverse = inverse_ref[...]
    body = slice(PAD, PAD + cols)
    low_y = jnp.where(even_y, yb[...], ya[...])
    high_y = jnp.where(even_y, ya[...], yb[...])
    low_c = jnp.where(even_x, cb[...], ca[...])
    high_c = jnp.where(even_x, ca[...], cb[...])
    pick = lambda one, two, n: jnp.where(even_x, one[n], two[n])
    sides = ((low_y, PAD - 2), (high_y, PAD + cols))
    ends = ((low_c, 0, xb, xa), (high_c, rows + 2, xa, xb))

    for r in range(rows + 4):
        for f in (f0, f1, f2):
            f[r, 0:PAD, :] = jnp.zeros((PAD, levels), jnp.float32)
            f[r, PAD + cols :, :] = jnp.zeros((PAD, levels), jnp.float32)
    for k, (f, ref) in enumerate(((f0, p0_ref), (f1, p1_ref), (f2, p2_ref))):
        for i in range(rows):
            f[i + 2, body, :] = ref[i]
        for _, at, one, two in ends:
            for n in range(2):
                f[at + n, body, :] = pick(one, two, 2 * k + n)
        for side, at in sides:
            for n in range(2):
                f[2 : rows + 2, at + n, :] = side[2 * k + n]
        if k < 2:
            for corner_rows, at, _, _ in ends:
                for m, (_, c) in enumerate(sides):
                    for n in range(2):
                        start = SIDE * m + 4 * k + 2 * n
                        for e in range(2):
                            f[at + e, c + n : c + n + 1, :] = corner_rows[start + e : start + e + 1]
    virtual = []
    for m, (c_rows, at, one, two) in enumerate(ends):
        outer = at + m
        virtual.append(f0[outer, body, :])
        for n, c in enumerate((PAD, PAD + cols - 2)):
            start = 2 * SIDE + 4 + 2 * n
            f0[outer, c : c + 2, :] = c_rows[start : start + 2]
    urows[...] = jnp.zeros_like(urows)
    for m, (c_rows, at, one, two) in enumerate(ends):
        outer, inner = ((0, 1), (3, 2))[m]
        urows[inner, body, :] = u_ref[0 if m == 0 else rows - 1]
        for s, (side, c) in enumerate(sides):
            urows[outer, c : c + 2, :] = c_rows[SIDE * s + 8 : SIDE * s + 10]
            urows[inner, c : c + 2, :] = side[7, 2 * m : 2 * m + 2]
    for s, (side, c) in enumerate(sides):
        outer, inner = ((0, 1), (3, 2))[s]
        vcols[outer, 2 : rows + 2, :] = side[6]
        vcols[inner, 2 : rows + 2, :] = v_ref[:, 0 if s == 0 else cols - 1, :]
        for c_rows, at, _, _ in ends:
            vcols[outer, at : at + 2, :] = c_rows[SIDE * s + 10 : SIDE * s + 12]
            vcols[inner, at : at + 2, :] = c_rows[2 * SIDE + 2 * s : 2 * SIDE + 2 * s + 2]

    cross(mu, f0, rows, cols)
    mu[2, body, :] += 0.25 * (virtual[0] - f0[0, body, :])
    mu[rows + 1, body, :] += 0.25 * (virtual[1] - f0[rows + 3, body, :])
    mu[1] -= 0.5 * urows[1]
    mu[2] += 0.5 * urows[0]
    mu[rows + 1] -= 0.5 * urows[3]
    mu[rows + 2] += 0.5 * urows[2]
    mu[:, PAD - 1, :] -= 0.5 * vcols[1]
    mu[:, PAD, :] += 0.5 * vcols[0]
    mu[:, PAD + cols - 1, :] -= 0.5 * vcols[3]
    mu[:, PAD + cols, :] += 0.5 * vcols[2]
    for c_rows, row in ((low_c, 2), (high_c, rows)):
        for s, c in enumerate((PAD - 4, PAD + cols + 2)):
            for n in range(2):
                start = SIDE * s + 16 + 2 * n
                for e in range(2):
                    mu[row + e, c + n : c + n + 1, :] = 0.25 * c_rows[start + e : start + e + 1]
    far = 0.25 * jnp.concatenate(
        [c_rows[SIDE * s + 12 : SIDE * s + 16] for c_rows in (low_c, high_c) for s in range(2)],
        axis=0,
    )
    far, _ = column_step(sound * far, None, sound, inside, inverse)
    far_out[...] = 0.25 * far

    for r in range(rows + 4):
        if 4 <= r < rows:
            spans = (slice(0, 2 * PAD), slice(cols, ext))
            clear = jnp.zeros((cols - 2 * PAD, levels), jnp.float32)
            for y in (yp, yw, yd):
                y[r, 2 * PAD : cols, :] = clear
        else:
            spans = (slice(0, ext),)
        for span in spans:
            d = -mu[r, span, :]
            q = -sound * d
            yp[r, span, :], yw[r, span, :] = column_step(
                q, None, sound, inside, inverse
            )
            yd[r, span, :] = d


def response_two(shape, sound_ref, inverse_ref, f0, f1, f2, yp, yw, yd, far_ref, *refs):
    s_out, yp_out, yw_out, yd_out, mu = refs
    rows, cols, levels = shape
    ext = cols + 2 * PAD
    sound = sound_ref[...]
    inside = interior(levels)
    inverse = inverse_ref[...]
    cross(mu, f1, rows, cols)
    for r in range(rows + 4):
        y = yp[r]
        near = pltpu.roll(y, 2, 0) + pltpu.roll(y, ext - 2, 0)
        if r >= 2:
            near += yp[r - 2]
        if r < rows + 2:
            near += yp[r + 2]
        mu[r] += 0.25 * near - y
        s_out[r] = f0[r] + f1[r] + y
    for m, at in enumerate((0, rows + 2)):
        for s, c in enumerate((PAD, PAD + cols - 2)):
            for n in range(2):
                start = 8 * m + 4 * s + 2 * n
                for e in range(2):
                    mu[at + e, c + n : c + n + 1, :] += far_ref[start + e : start + e + 1, :]
    for r in range(rows + 4):
        d = yd[r] - mu[r]
        p, w = column_step(yp[r] - sound * d, yw[r], sound, inside, inverse)
        yd_out[r] = d
        yp_out[r] = p
        yw_out[r] = w
        s_out[r] += f2[r] + p


def response_three(sound_ref, inverse_ref, u_ref, v_ref, p3_ref, w3_ref, f2, *refs):
    s_ref, yp, yw, yd, u_final, v_final, w_out, p_out, mu, u_out, v_out, sems = refs
    moves = [
        pltpu.make_async_copy(u_out, u_final, sems.at[0]),
        pltpu.make_async_copy(v_out, v_final, sems.at[1]),
    ]
    rows, cols, levels = u_ref.shape
    sound = sound_ref[...]
    inside = interior(levels)
    inverse = inverse_ref[...]
    body = slice(PAD, PAD + cols)
    for i in range(rows):
        r = i + 2
        u_out[i] = u_ref[i] - 0.5 * (s_ref[r + 1, body, :] - s_ref[r - 1, body, :])
        east = lambda n: s_ref[r, PAD + n : PAD + n + cols, :]
        v_out[i] = v_ref[i] - 0.5 * (east(1) - east(-1))
    for move in moves:
        move.start()
    cross(mu, f2, rows, cols)
    for i in range(rows):
        r = i + 2
        d = yd[r, body, :] - mu[r, body, :] - bend(yp, r, cols)
        p, w = column_step(
            yp[r, body, :] - sound * d, yw[r, body, :], sound, inside, inverse
        )
        p_out[i] = p3_ref[i] + p
        w_out[i] = w3_ref[i] + w
    for move in moves:
        move.wait()


def settle_kernel(columns, p_ref, w_ref, drift_ref, sums_ref, w_out, p_out, profile_out):
    rows, _, levels = p_ref.shape
    total = sums_ref[...] * (1.0 / columns)
    profile_out[...] = total[0:1]
    mean = jnp.broadcast_to(total[1:2], (8, levels))
    drift = exact_dot(mean, drift_ref[...])
    for i in range(rows):
        p_out[i] = p_ref[i] + drift[0:1, 0:levels]
        w_out[i] = w_ref[i] + drift[0:1, levels:]


def response(kernel, args, outs, scratch, flops, direct=0):
    return pl.pallas_call(
        kernel,
        in_specs=[VMEM] * len(args),
        out_specs=[pl.BlockSpec(memory_space=pltpu.HBM)] * direct + [VMEM] * (len(outs) - direct),
        out_shape=outs,
        scratch_shapes=scratch,
        compiler_params=pltpu.CompilerParams(vmem_limit_bytes=GRANT),
        cost_estimate=pl.CostEstimate(flops=flops, bytes_accessed=6_000_000, transcendentals=0),
    )(*args)


def swaps(count):
    near = [(i, i ^ 1) for i in range(count)]
    far = [(i, (i + 1) % count if i % 2 else (i - 1) % count) for i in range(count)]
    return near, far


def exchange(a, b, axis):
    near, far = swaps(lax.axis_size(axis))
    a = lax.ppermute(a, axis, near)
    b = lax.ppermute(b, axis, far)
    return a, b


def total_sum(value, axis):
    count = lax.axis_size(axis)
    distance = 2
    while distance < count:
        moved = lax.ppermute(value, axis, [(i, i ^ distance) for i in range(count)])
        value = value + moved
        distance *= 2
    return value


def window(
    eastward,
    northward,
    vertical,
    pressure,
    theta,
    humidity,
    sound_speed,
    radius_sq,
    multiplicity,
    droplet_count,
):
    columns = float(theta.shape[0] * theta.shape[1] * lax.axis_size("gx") * lax.axis_size("gy"))
    sound = sound_speed[None]
    (
        theta_out,
        humidity_out,
        radius_out,
        sums,
        weights,
        p1,
        p2,
        w2,
        d2,
        heat,
        xa,
        xb,
        ya,
        yb,
        edge,
    ) = first(
        *(
            pltpu.with_memory_space_constraint(x, pltpu.HBM)
            for x in (
                sound,
                theta,
                humidity,
                radius_sq,
                multiplicity,
                droplet_count,
                pressure,
                eastward,
                northward,
                vertical,
            )
        )
    )
    rows, cols, levels = theta.shape
    f32 = lambda *shape: jax.ShapeDtypeStruct(shape, jnp.float32)
    wide = (rows + 4, cols + 2 * PAD, levels)
    xa, xb = exchange(xa, xb, "gx")
    ya, yb = exchange(ya, yb, "gy")
    sums = total_sum(sums + ya[9, 0:2], "gy")
    ca, cb = corner(ya, yb, edge, sums)
    ca, cb = exchange(ca, cb, "gx")
    at = 2 * SIDE + 8
    sums = total_sum(sums + ca[at : at + 2], "gx")
    p3, w3, drift = third(sound, weights, heat, p2, w2, d2)
    f0, f1, f2, yp, yw, yd, far = response(
        functools.partial(response_one, ("gx", "gy")),
        (sound, weights, pressure, eastward, northward, p1, p2, xa, xb, ya, yb, ca, cb),
        [f32(*wide)] * 6 + [f32(16, levels)],
        [
            pltpu.VMEM(wide, jnp.float32),
            pltpu.VMEM((4, cols + 2 * PAD, levels), jnp.float32),
            pltpu.VMEM((4, rows + 4, levels), jnp.float32),
        ],
        4_000_000_000,
    )
    moved, yp, yw, yd = response(
        functools.partial(response_two, theta.shape),
        (sound, weights, f0, f1, f2, yp, yw, yd, far),
        [f32(*wide)] * 4,
        [pltpu.VMEM(wide, jnp.float32)],
        4_000_000_000,
    )
    u, v, w, p = response(
        response_three,
        (sound, weights, eastward, northward, p3, w3, f2, moved, yp, yw, yd),
        [f32(*theta.shape)] * 4,
        [pltpu.VMEM(wide, jnp.float32)]
        + [pltpu.VMEM(theta.shape, jnp.float32)] * 2
        + [pltpu.SemaphoreType.DMA((2,))],
        4_000_000_000,
        direct=2,
    )
    w, p, profile = response(
        functools.partial(settle_kernel, columns),
        (p, w, drift, sums),
        [f32(*theta.shape)] * 2 + [f32(1, levels)],
        [],
        100_000_000,
    )
    return (u, v, w, p, theta_out, humidity_out, radius_out, profile[0])


def solution(mesh):
    grid = P("gx", "gy", None)
    drops = P(None, None, "gx", "gy")
    return jax.shard_map(
        window,
        mesh=mesh,
        in_specs=(grid,) * 6 + (P(), drops, drops, P(None, "gx", "gy")),
        out_specs=(grid,) * 6 + (drops, P()),
        check_vma=False,
    )
```
